256 devices in a mesh: tm: 32 (over z, y), mp: 4 (over x), dec: 2 (over core).
Axes of the slice: x: 4, y: 4, z: 8, core: 2. Of those that a mesh axis runs over, the one named last changes fastest.
Arguments:
- latents: bfloat16 [8192, 3072], P('tm'), may hold values from -6 to 6
- modulation: float32 [32, 3, 3072], P('tm'), may hold values from -1.5 to 3.5
- w_qkv: bfloat16 [3, 3072, 3072], P(None, None, ('mp', 'dec'))
- w_out: bfloat16 [3072, 3072], P(('mp', 'dec')), may hold values from -0.109375 to 0.109375
- block_mask: int32 [32, 32], replicated, may hold values from 0 to 1, as said below
- lengths: int32 [32], replicated, may hold values from 64 to 256, as said below
Outputs:
- updated: bfloat16 [8192, 3072], P('tm', ('mp', 'dec'))
The draws below stay inside these ranges and needn't reach their ends.
Inputs may be any that keep to these rules, and one draw needn't show every extreme that they name: block_mask[i, i] = 1 and block_mask[i, j] = 0 for j > i. `lengths`: some group of index 16 or more has all 256 tokens live.
All inputs are finite; a program needn't handle non-finite values.
Results may differ from the reference program's by a relative error of at most 0.0057.
Values may be sent and summed in bfloat16 or wider, within the bound.
A program may use at most 192 MiB of HBM per device.

```python
import jax
import jax.numpy as jnp
from jax import lax

D = 3072
HEADS = 24
HS = 128
TOK = 256
GROUPS = 32
TOKENS = 8192
N_TM = 32


def causal_pattern(key):
    coins = jax.random.randint(key, (GROUPS, GROUPS), 0, 5) > 0
    rows_index = jnp.arange(GROUPS, dtype=jnp.int32)[:, None]
    cols_index = jnp.arange(GROUPS, dtype=jnp.int32)[None, :]
    below = jnp.where(coins, 1, 0).astype(jnp.int32)
    return jnp.where(rows_index == cols_index, 1, jnp.where(cols_index < rows_index, below, 0)).astype(jnp.int32)


def full_group(key):
    second = jax.random.fold_in(key, 1)
    return jax.random.randint(second, (), GROUPS // 2, GROUPS).astype(jnp.int32)


def draw_modulation(key, part):
    first = jax.random.fold_in(key, 0)
    base = jnp.clip(0.5 * jax.random.normal(first, (GROUPS, 3, D), jnp.float32), -1.5, 1.5)
    return base


def draw_w_qkv(key, part):
    first = jax.random.fold_in(key, 0)
    scale = D ** (-0.5)
    weights = jnp.clip(jax.random.normal(first, (3, D, HEADS * HS), jnp.float32), -4.0, 4.0) * scale
    return weights.astype(jnp.bfloat16)


def draw_block_mask(key, part):
    return causal_pattern(key)


def draw_lengths(key, part):
    first = jax.random.fold_in(key, 0)
    drawn = jax.random.randint(first, (GROUPS,), TOK // 4, TOK + 1)
    target = full_group(key)
    return drawn.at[target].set(TOK).astype(jnp.int32)


def block_levels(key, dims, shards, smallest, top_value):
    level, own = 1.0, jax.random.fold_in(key, 6)
    for axis_at, shards_of in shards:
        draws = jnp.exp(jax.random.uniform(jax.random.fold_in(own, axis_at), (shards_of,), jnp.float32, smallest / len(shards), top_value / len(shards)))
        level = level * jnp.repeat(draws, dims[axis_at] // shards_of).reshape([-1 if axis == axis_at else 1 for axis in range(len(dims))])
    return level


def gaussian(rng, dims, scale, bound, pieces=(), held_as=jnp.bfloat16):
    loudness = block_levels(rng, dims, pieces, -0.22, 0.18) if pieces else 1.0
    array = jax.random.normal(rng, dims, jnp.float32) * scale * loudness
    return jnp.minimum(jnp.maximum(array, -bound), bound).astype(held_as)


def setup_inputs(seed: int = 0) -> dict:
    streams_of = jax.random.split(jax.random.key(seed), 7)
    latents = gaussian(streams_of[0], (TOKENS, D), 1.0, 6.0, ((0, 32),))
    modulation = draw_modulation(jax.random.fold_in(streams_of[6], 71), 0)
    w_qkv = draw_w_qkv(jax.random.fold_in(streams_of[6], 71), 0)
    w_out = gaussian(streams_of[3], (HEADS * HS, D), (HEADS * HS) ** -0.5, 0.109375, ((0, 8),))
    block_mask = draw_block_mask(jax.random.fold_in(streams_of[6], 71), 0)
    lengths = draw_lengths(jax.random.fold_in(streams_of[6], 71), 0)
    return dict(latents=latents, modulation=modulation, w_qkv=w_qkv, w_out=w_out, block_mask=block_mask, lengths=lengths)


def reference(latents, modulation, w_qkv, w_out, block_mask, lengths):
    wide = latents.astype(jnp.float32)
    mean = lax.optimization_barrier(jnp.mean(wide, axis=-1, keepdims=True))
    var = lax.optimization_barrier(jnp.mean((wide - mean) ** 2, axis=-1, keepdims=True))
    normed = (wide - mean) * lax.rsqrt(var + 1e-06)
    per_token = jnp.repeat(modulation, TOK, axis=0)
    adapted = (normed * (1.0 + per_token[:, 1]) + per_token[:, 0]).astype(jnp.bfloat16)
    query = jnp.dot(adapted, w_qkv[0], preferred_element_type=jnp.float32).astype(jnp.bfloat16)
    key = jnp.dot(adapted, w_qkv[1], preferred_element_type=jnp.float32).astype(jnp.bfloat16)
    value = jnp.dot(adapted, w_qkv[2], preferred_element_type=jnp.float32).astype(jnp.bfloat16)
    slots = jnp.arange(TOKENS, dtype=jnp.int32)
    key_group = slots // TOK
    key_live = slots % TOK < lengths[key_group]
    key_all = key.astype(jnp.float32).reshape(TOKENS, HEADS, HS)
    value_all = value.astype(jnp.float32).reshape(TOKENS, HEADS, HS)

    def one_group(group):
        rows = lax.dynamic_slice_in_dim(query, group * TOK, TOK, 0)
        rows = rows.astype(jnp.float32).reshape(TOK, HEADS, HS)
        score = jnp.einsum('thd,shd->hts', rows, key_all) / jnp.sqrt(jnp.float32(HS))
        allowed = (block_mask[group][key_group] == 1) & key_live
        score = jnp.where(allowed[None, None, :], score, jnp.float32(-1e+30))
        peak = lax.optimization_barrier(jnp.max(score, axis=-1, keepdims=True))
        weight = jnp.exp(score - peak) * allowed[None, None, :].astype(jnp.float32)
        total = lax.optimization_barrier(jnp.sum(weight, axis=-1))
        weight_b = lax.optimization_barrier(weight.astype(jnp.bfloat16)).astype(jnp.float32)
        mixed = jnp.einsum('hts,shd->thd', weight_b, value_all)
        mixed = mixed / jnp.transpose(total)[:, :, None]
        return mixed.reshape(TOK, HEADS * HS).astype(jnp.bfloat16)
    attended = lax.map(one_group, jnp.arange(N_TM, dtype=jnp.int32)).reshape(TOKENS, HEADS * HS)
    branch = jnp.dot(attended, w_out, preferred_element_type=jnp.float32)
    return (wide + per_token[:, 2] * branch).astype(jnp.bfloat16)
```

```python
import jax
import jax.numpy as jnp
from jax import lax
from jax.experimental import pallas as pl
from jax.experimental.pallas import tpu as pltpu
from jax.sharding import PartitionSpec as P

HS = 128
TOK = 256
NZ, NY, NX = 8, 4, 4
NEG = -1e30
LOG2E = 1.4426950408889634
HALF = TOK // 2


def rem(a, b):
    return lax.rem(a, jnp.int32(b))


def div(a, b):
    return lax.div(a, jnp.int32(b))


def kernel(
    lat_hbm, mod_hbm, wqkv_hbm, wout_hbm, mask_ref, len_ref, out_ref,
    lat, mod, adapted, wkv, wq, kvsend, qsend, kv, q, acc, mx, sm, attsend, att, wcol,
    in_sem, wkv_sem, kvs_sem, qs_sem, kv_sem, q_sem, b_sem, c_sem, att_sem, x_sem, wos_sem, wor_sem,
):
    t_id = lax.axis_index("tm")
    z, y = div(t_id, NY), rem(t_id, NY)
    m = lax.axis_index("mp")
    c = lax.axis_index("dec")
    yp, ym, y2 = rem(y + 1, NY), rem(y + NY - 1, NY), rem(y + 2, NY)
    xp, xm, x2 = rem(m + 1, NX), rem(m + NX - 1, NX), rem(m + 2, NX)
    width = wout_hbm.shape[0]
    row_core = div(z, 4)
    row_u = 3 * row_core + rem(z, 4)
    active = rem(z, 4) != 3

    def at(z_=z, y_=y, m_=m, c_=c):
        return {"tm": z_ * NY + y_, "mp": m_, "dec": c_}

    def remote(src, dst, ssem, rsem, device):
        return pltpu.make_async_remote_copy(
            src_ref=src, dst_ref=dst, send_sem=ssem, recv_sem=rsem,
            device_id=device, device_id_type=pl.DeviceIdType.MESH,
        )

    lat_copy = pltpu.make_async_copy(lat_hbm, lat, in_sem.at[0])
    mod_copy = pltpu.make_async_copy(mod_hbm.at[0], mod, in_sem.at[1])
    lat_copy.start()
    mod_copy.start()

    def weight_copy(k, part):
        cols = pl.ds(pl.multiple_of(k * HS, HS), HS)
        return pltpu.make_async_copy(
            wqkv_hbm.at[1 + part, :, cols], wkv.at[k, :, pl.ds(part * HS, HS)], wkv_sem.at[k, part]
        )

    for k in range(3):
        for part in range(2):
            weight_copy(k, part).start()
    wq_copy = pltpu.make_async_copy(wqkv_hbm.at[0], wq, in_sem.at[2])
    wq_copy.start()
    own_cols = pl.ds(pl.multiple_of((2 * m + c) * width, HS), width)
    own_rows = pl.ds(pl.multiple_of(c * width, HS), width)
    wout_copy = pltpu.make_async_copy(wout_hbm.at[:, own_cols], wcol.at[m, own_rows, :], in_sem.at[3])
    wout_copy.start()

    barrier = pltpu.get_barrier_semaphore()
    partners = [at(c_=1 - c), at(y_=yp), at(y_=ym)]
    for dz in range(1, NZ):
        for cc in range(2):
            partners.append(at(z_=rem(z + dz, NZ), c_=jnp.int32(cc)))
    for dx in range(1, NX):
        for cc in range(2):
            partners.append(at(m_=rem(m + dx, NX), c_=jnp.int32(cc)))
    for device in partners:
        pl.semaphore_signal(barrier, inc=1, device_id=device, device_id_type=pl.DeviceIdType.MESH)

    lat_copy.wait()
    mod_copy.wait()
    rows = 16

    @pl.loop(0, TOK // rows)
    def _(r):
        block = pl.ds(pl.multiple_of(r * rows, rows), rows)
        wide = lat[block, :].astype(jnp.float32)
        centred = wide - jnp.mean(wide, axis=-1, keepdims=True)
        var = jnp.mean(centred * centred, axis=-1, keepdims=True)
        normed = centred * lax.rsqrt(var + 1e-06)
        adapted[block, :] = (normed * (1.0 + mod[1:2, :]) + mod[0:1, :]).astype(jnp.bfloat16)

    pl.semaphore_wait(barrier, len(partners))

    def wout_sends():
        copies = []
        for dx in range(NX):
            for dc in range(2):
                if dx == 0 and dc == 0:
                    continue
                m_, c_ = rem(m + dx, NX), rem(c + dc, 2)
                cols = pl.ds(pl.multiple_of((2 * m_ + c_) * width, HS), width)
                copies.append(remote(
                    wout_hbm.at[:, cols], wcol.at[m, own_rows, :],
                    wos_sem.at[dx, dc], wor_sem.at[dx, dc], at(m_=m_, c_=c_),
                ))
        return copies

    for copy in wout_sends():
        copy.start()

    def piece(s, p, start=0, size=TOK):
        return kv.at[s, pl.ds(pl.multiple_of(p * TOK + start, HALF), size), :]

    q_core = rem(div(z + 1, 2), 2)
    slab_core = rem(z, 2)

    def kv_remote(k):
        return remote(kvsend.at[k], piece(z, y), kvs_sem.at[k], kv_sem.at[z, y, 0], at(z_=4 * c + k, c_=slab_core))

    def q_remote(k):
        return remote(qsend.at[k], q.at[div(z, 2)], qs_sem.at[k], q_sem.at[div(z, 2)], at(z_=4 * c + k, c_=q_core))

    @pl.loop(0, 3)
    def _(k):
        weight_copy(k, 0).wait()
        weight_copy(k, 1).wait()
        made = jnp.dot(adapted[...], wkv[k], preferred_element_type=jnp.float32).astype(jnp.bfloat16)
        here = (4 * c + k == z) & (slab_core == c)

        @pl.when(here)
        def _():
            kv[z, pl.ds(pl.multiple_of(y * TOK, TOK), TOK), :] = made

        @pl.when(jnp.logical_not(here))
        def _():
            kvsend[k] = made
            kv_remote(k).start()

    wq_copy.wait()
    made_q = jnp.dot(adapted[...], wq[...], preferred_element_type=jnp.float32) * (LOG2E / HS**0.5)
    made_q = made_q.astype(jnp.bfloat16)
    for k in range(3):
        here = (4 * c + k == z) & (q_core == c)
        one = made_q[:, k * HS:(k + 1) * HS]

        @pl.when(here)
        def _():
            q[div(z, 2)] = one

        @pl.when(jnp.logical_not(here))
        def _():
            qsend[k] = one
            q_remote(k).start()

    def order(t):
        return rem(z + (1 - 2 * rem(t, 2)) * div(t + 1, 2) + NZ, NZ)

    def group_row(k):
        return 2 * k + rem(k + c, 2)

    def kv_wait(s, p, half=0, size=TOK):
        start = half * HALF if size == HALF else 0
        ref = piece(s, p, start, size)
        remote(ref, ref, b_sem.at[s, 0], kv_sem.at[s, p, half], at(c_=1 - c)).wait_recv()

    def hop(s, p, slot, device, half=None):
        start, size = (0, TOK) if half is None else (half * HALF, HALF)
        ref = piece(s, p, start, size)
        return remote(ref, ref, b_sem.at[s, slot], kv_sem.at[s, p, half or 0], device)

    def hops(s):
        up, down, across = at(y_=yp), at(y_=ym), at(c_=1 - c)
        return [
            hop(s, y, 0, up), hop(s, y, 1, down), hop(s, y, 2, across),
            hop(s, ym, 3, up, 0), hop(s, ym, 4, across),
            hop(s, yp, 5, down, 1), hop(s, yp, 6, across),
            hop(s, y2, 7, across),
        ]

    def tile(k, s):
        group = group_row(k) * NY + y
        lane = lax.broadcasted_iota(jnp.int32, (1, TOK), 1)
        parts = []
        for p in range(NY):
            key_group = s * NY + p
            limit = jnp.where(mask_ref[group, key_group] == 1, len_ref[key_group], 0)
            parts.append(jnp.where(lane < limit, 0.0, NEG).astype(jnp.float32))
        bias = jnp.concatenate(parts, axis=1)
        score = lax.dot_general(
            q[k], kv[s, :, 0:HS], (((1,), (1,)), ((), ())), preferred_element_type=jnp.float32
        ) + bias
        old = mx[k]
        new = jnp.maximum(old, jnp.max(score, axis=-1, keepdims=True))
        keep = jnp.exp2(old - new)
        weight = jnp.exp2(score - new[:, 0:1])
        mx[k] = new
        sm[k] = sm[k] * keep + jnp.sum(weight, axis=-1, keepdims=True)
        acc[k] = acc[k] * keep + jnp.dot(
            weight.astype(jnp.bfloat16), kv[s, :, HS:2 * HS], preferred_element_type=jnp.float32
        )

    def att_piece(x, u, half=None):
        start, size = (0, TOK) if half is None else (half * HALF, HALF)
        return att.at[x, pl.ds(start, size), pl.ds(pl.multiple_of(u * HS, HS), HS)]

    def att_remote(k):
        return remote(
            attsend.at[k], att_piece(m, row_u), c_sem.at[k], att_sem.at[m, row_u, 0],
            at(z_=group_row(k), c_=row_core),
        )

    def q_here(k):
        return (group_row(k) == z) & (row_core == c)

    @pl.when(active)
    def _():
        mx[...] = jnp.full(mx.shape, NEG, jnp.float32)
        sm[...] = jnp.zeros(sm.shape, jnp.float32)
        acc[...] = jnp.zeros(acc.shape, jnp.float32)

        @pl.loop(0, NZ + 3)
        def _(t):
            @pl.when(t < NZ)
            def _():
                s = order(t)

                @pl.when(rem(s, 2) == c)
                def _():
                    @pl.when(jnp.logical_not((t == 0) & (row_core == c)))
                    def _():
                        kv_wait(s, y)

                    for copy in hops(s)[0:3]:
                        copy.start()

            @pl.when((t >= 1) & (t < NZ + 1))
            def _():
                s = order(t - 1)

                @pl.when(rem(s, 2) == c)
                def _():
                    kv_wait(s, ym)
                    for copy in hops(s)[3:5]:
                        copy.start()
                    kv_wait(s, yp)
                    for copy in hops(s)[5:7]:
                        copy.start()

            @pl.when((t >= 2) & (t < NZ + 2))
            def _():
                s = order(t - 2)

                @pl.when(rem(s, 2) == c)
                def _():
                    kv_wait(s, y2, 0, HALF)
                    kv_wait(s, y2, 1, HALF)
                    hops(s)[7].start()

            @pl.when(t >= 3)
            def _():
                s = order(t - 3)

                @pl.when(rem(s, 2) != c)
                def _():
                    for p in range(NY):
                        kv_wait(s, jnp.int32(p))

                @pl.when(t == 3)
                def _():
                    for k in range(4):
                        @pl.when(jnp.logical_not(q_here(jnp.int32(k))))
                        def _():
                            remote(q.at[k], q.at[k], c_sem.at[k], q_sem.at[k], at(c_=1 - c)).wait_recv()

                @pl.loop(0, 4)
                def _(k):
                    @pl.when(s <= group_row(k))
                    def _():
                        tile(k, s)

                    @pl.when(t == NZ + 2)
                    def _():
                        done = (acc[k] / sm[k]).astype(jnp.bfloat16)

                        @pl.when(q_here(k))
                        def _():
                            att[m, :, pl.ds(pl.multiple_of(row_u * HS, HS), HS)] = done

                        @pl.when(jnp.logical_not(q_here(k)))
                        def _():
                            attsend[k] = done
                            att_remote(k).start()

    def att_wait(x, u, half=None):
        ref = att_piece(x, u, half)
        remote(ref, ref, x_sem.at[0, 0], att_sem.at[x, u, half or 0], at(c_=1 - c)).wait_recv()

    def att_hop(x, u, k, slot, device, half=None):
        ref = att_piece(x, u, half)
        return remote(ref, ref, x_sem.at[k, slot], att_sem.at[x, u, half or 0], device)

    def att_hops(k):
        u = 3 * c + k
        up, down, across = at(m_=xp), at(m_=xm), at(c_=1 - c)
        return [
            att_hop(m, u, k, 0, up), att_hop(m, u, k, 1, down), att_hop(m, u, k, 2, across),
            att_hop(xm, u, k, 3, up, 0), att_hop(xm, u, k, 4, across),
            att_hop(xp, u, k, 5, down, 1), att_hop(xp, u, k, 6, across),
            att_hop(x2, u, k, 7, across),
        ]

    @pl.loop(0, 3)
    def _(k):
        @pl.when(jnp.logical_not((4 * c + k == z) & (q_core == c)))
        def _():
            att_wait(m, 3 * c + k)

        for copy in att_hops(k)[0:3]:
            copy.start()

    @pl.loop(0, 3)
    def _(k):
        att_wait(xm, 3 * c + k)
        for copy in att_hops(k)[3:5]:
            copy.start()
        att_wait(xp, 3 * c + k)
        for copy in att_hops(k)[5:7]:
            copy.start()

    @pl.loop(0, 3)
    def _(k):
        att_wait(x2, 3 * c + k, 0)
        att_wait(x2, 3 * c + k, 1)
        att_hops(k)[7].start()

    wout_copy.wait()
    for copy in wout_sends():
        copy.wait_recv()
    for x in range(NX):
        for k in range(3):
            att_wait(jnp.int32(x), 3 * (1 - c) + k)

    branch = jnp.dot(att[0], wcol[0], preferred_element_type=jnp.float32)
    for x in range(1, NX):
        branch += jnp.dot(att[x], wcol[x], preferred_element_type=jnp.float32)
    wide = lat[:, own_cols].astype(jnp.float32)
    out_ref[...] = (wide + mod[2:3, own_cols] * branch).astype(jnp.bfloat16)

    for copy in wout_sends():
        copy.wait_send()

    @pl.loop(0, 3)
    def _(k):
        @pl.when(jnp.logical_not((4 * c + k == z) & (slab_core == c)))
        def _():
            kv_remote(k).wait_send()

        @pl.when(jnp.logical_not((4 * c + k == z) & (q_core == c)))
        def _():
            q_remote(k).wait_send()

        for copy in att_hops(k):
            copy.wait_send()

    @pl.when(active)
    def _():
        @pl.loop(0, NZ)
        def _(s):
            @pl.when(rem(s, 2) == c)
            def _():
                for copy in hops(s):
                    copy.wait_send()

        @pl.loop(0, 4)
        def _(k):
            @pl.when(jnp.logical_not(q_here(k)))
            def _():
                att_remote(k).wait_send()


def shards(latents, modulation, w_qkv, w_out, block_mask, lengths):
    tok, d = latents.shape
    width = w_out.shape[0]
    dma = pltpu.SemaphoreType.DMA
    vmem = pltpu.VMEM
    bf16, f32 = jnp.bfloat16, jnp.float32
    anywhere = pl.BlockSpec(memory_space=pl.ANY)
    scalars = pl.BlockSpec(memory_space=pltpu.SMEM)
    return pl.pallas_call(
        kernel,
        out_shape=jax.ShapeDtypeStruct((tok, width), bf16),
        in_specs=[anywhere] * 4 + [scalars] * 2,
        out_specs=pl.BlockSpec(memory_space=pltpu.VMEM),
        scratch_shapes=[
            vmem((tok, d), bf16), vmem((3, d), f32), vmem((tok, d), bf16),
            vmem((3, d, 2 * HS), bf16), vmem((d, width), bf16),
            vmem((3, tok, 2 * HS), bf16), vmem((3, tok, HS), bf16),
            vmem((NZ, NY * tok, 2 * HS), bf16), vmem((4, tok, HS), bf16),
            vmem((4, tok, HS), f32), vmem((4, tok, HS), f32), vmem((4, tok, HS), f32),
            vmem((4, tok, HS), bf16), vmem((NX, tok, 6 * HS), bf16), vmem((NX, 2 * width, width), bf16),
            dma((4,)), dma((3, 2)), dma((3,)), dma((3,)), dma((NZ, NY, 2)), dma((4,)),
            dma((NZ, 8)), dma((4,)), dma((NX, 6, 2)), dma((3, 8)), dma((NX, 2)), dma((NX, 2)),
        ],
        compiler_params=pltpu.CompilerParams(
            collective_id=0, has_side_effects=True, vmem_limit_bytes=60 * 1024 * 1024
        ),
        name="attention_sublayer",
    )(latents, modulation, w_qkv, w_out, block_mask, lengths)


def solution(mesh):
    return jax.shard_map(
        shards,
        mesh=mesh,
        in_specs=(
            P("tm", None),
            P("tm", None, None),
            P(None, None, ("mp", "dec")),
            P(("mp", "dec"), None),
            P(),
            P(),
        ),
        out_specs=P("tm", ("mp", "dec")),
        check_vma=False,
    )
```

```python
import jax
import jax.numpy as jnp
from jax import lax
from jax.experimental import pallas as pl
from jax.experimental.pallas import tpu as pltpu
from jax.sharding import PartitionSpec as P

HS = 128
TOK = 256
NZ, NY, NX = 8, 4, 4
NEG = -1e30
LOG2E = 1.4426950408889634
HALF = TOK // 2
PAUSE = 2500


def rem(a, b):
    return lax.rem(a, jnp.int32(b))


def div(a, b):
    return lax.div(a, jnp.int32(b))


def kernel(
    lat_hbm, mod_hbm, wqkv_hbm, wout_hbm, mask_ref, len_ref, out_ref,
    lat, mod, adapted, wqkv, kvsend, qsend, kv, q, acc, mx, sm, attsend, att, wcol, branch,
    in_sem, w_sem, kvs_sem, qs_sem, kv_sem, q_sem, b_sem, c_sem, att_sem, x_sem, wos_sem, wor_sem,
):
    t_id = lax.axis_index("tm")
    z, y = div(t_id, NY), rem(t_id, NY)
    m = lax.axis_index("mp")
    c = lax.axis_index("dec")
    yp, ym, y2 = rem(y + 1, NY), rem(y + NY - 1, NY), rem(y + 2, NY)
    xp, xm, x2 = rem(m + 1, NX), rem(m + NX - 1, NX), rem(m + 2, NX)
    width = wout_hbm.shape[0]
    row_core = div(z, 4)
    row_u = 3 * row_core + rem(z, 4)
    active = rem(z, 4) != 3
    q_core = rem(div(z + 1, 2), 2)
    slab_core = rem(z, 2)

    rel = rem(z - 4 * c + NZ, NZ)
    first = jnp.where(rel == 1, 1, jnp.where((rel >= 2) & (rel <= 4), 2, 0))
    second = jnp.where(rel == 1, 0, jnp.where(rel == 5, 2, 1))

    def nearest(i):
        return jnp.where(i == 0, first, jnp.where(i == 1, second, 3 - first - second))

    def at(z_=z, y_=y, m_=m, c_=c):
        return {"tm": z_ * NY + y_, "mp": m_, "dec": c_}

    def remote(src, dst, ssem, rsem, device):
        return pltpu.make_async_remote_copy(
            src_ref=src, dst_ref=dst, send_sem=ssem, recv_sem=rsem,
            device_id=device, device_id_type=pl.DeviceIdType.MESH,
        )

    lat_copy = pltpu.make_async_copy(lat_hbm, lat, in_sem.at[0])
    mod_copy = pltpu.make_async_copy(mod_hbm, mod, in_sem.at[1])
    lat_copy.start()
    mod_copy.start()

    barrier = pltpu.get_barrier_semaphore()
    partners = [at(c_=1 - c), at(y_=yp), at(y_=ym)]
    for dz in range(1, NZ):
        for cc in range(2):
            partners.append(at(z_=rem(z + dz, NZ), c_=jnp.int32(cc)))
    for dx in range(1, NX):
        for cc in range(2):
            partners.append(at(m_=rem(m + dx, NX), c_=jnp.int32(cc)))
    for device in partners:
        pl.semaphore_signal(barrier, inc=1, device_id=device, device_id_type=pl.DeviceIdType.MESH)

    def weight_copy(k, part):
        cols = pl.ds(pl.multiple_of(k * HS, HS), HS)
        return pltpu.make_async_copy(
            wqkv_hbm.at[(part + 1) % 3, :, cols], wqkv.at[k, :, pl.ds(part * HS, HS)], w_sem.at[k, part]
        )

    for i in range(3):
        for part in range(3):
            weight_copy(nearest(i), part).start()
    own_cols = pl.ds(pl.multiple_of((2 * m + c) * width, HS), width)
    own_rows = pl.ds(pl.multiple_of(c * width, HS), width)
    wout_copy = pltpu.make_async_copy(wout_hbm.at[:, own_cols], wcol.at[m, own_rows, :], in_sem.at[2])
    wout_copy.start()

    mx[...] = jnp.full(mx.shape, NEG, jnp.float32)
    sm[...] = jnp.zeros(sm.shape, jnp.float32)
    acc[...] = jnp.zeros(acc.shape, jnp.float32)

    with jax.named_scope("load"):
        lat_copy.wait()
        mod_copy.wait()
    rows = 16

    @pl.loop(0, TOK // rows, unroll=4)
    def _(r):
        block = pl.ds(pl.multiple_of(r * rows, rows), rows)
        wide = lat[block, :].astype(jnp.float32)
        centred = wide - jnp.mean(wide, axis=-1, keepdims=True)
        var = jnp.mean(centred * centred, axis=-1, keepdims=True)
        normed = centred * lax.rsqrt(var + 1e-06)
        adapted[block, :] = (normed * (1.0 + mod[1]) + mod[0]).astype(jnp.bfloat16)

    with jax.named_scope("entry"):
        pl.semaphore_wait(barrier, len(partners))

    def wout_send(dx, dc):
        m_, c_ = rem(m + dx, NX), rem(c + dc, 2)
        cols = pl.ds(pl.multiple_of((2 * m_ + c_) * width, HS), width)
        return remote(
            wout_hbm.at[:, cols], wcol.at[m, own_rows, :],
            wos_sem.at[0], wor_sem.at[dx, dc], at(m_=m_, c_=c_),
        )

    others = [(dx, dc) for dx in range(NX) for dc in range(2) if (dx, dc) != (0, 0)]

    def piece(s, p, start=0, size=TOK):
        return kv.at[s, pl.ds(pl.multiple_of(p * TOK + start, HALF), size), :]

    def kv_remote(k):
        return remote(kvsend.at[k], piece(z, y), kvs_sem.at[k], kv_sem.at[z, y, 0], at(z_=4 * c + k, c_=slab_core))

    def q_remote(k):
        return remote(qsend.at[k], q.at[div(z, 2)], qs_sem.at[k], q_sem.at[div(z, 2)], at(z_=4 * c + k, c_=q_core))

    def kv_local(k):
        return (4 * c + k == z) & (slab_core == c)

    def q_local(k):
        return (4 * c + k == z) & (q_core == c)

    def send_phase(phase, i):
        k = nearest(i)
        away = rem(4 * c + k - z + NZ, NZ)
        far = jnp.maximum(jnp.minimum(away, NZ - away), 1)

        @pl.when((far == phase) & jnp.logical_not(kv_local(k)))
        def _():
            kv_remote(k).start()

        @pl.when((jnp.maximum(far - 1, 1) == phase) & jnp.logical_not(q_local(k)))
        def _():
            q_remote(k).start()

    def send_rest(phase):
        @pl.loop(0, 3)
        def _(i):
            send_phase(phase, i)

    @pl.loop(0, 3)
    def _(i):
        k = nearest(i)
        with jax.named_scope("weights"):
            for part in range(3):
                weight_copy(k, part).wait()
        made = jnp.dot(adapted[...], wqkv[k], preferred_element_type=jnp.float32)
        kvsend[k] = made[:, 0:2 * HS].astype(jnp.bfloat16)
        qsend[k] = (made[:, 2 * HS:3 * HS] * (LOG2E / HS**0.5)).astype(jnp.bfloat16)

        @pl.when(kv_local(k))
        def _():
            kv[z, pl.ds(pl.multiple_of(y * TOK, TOK), TOK), :] = kvsend[k]

        @pl.when(q_local(k))
        def _():
            q[div(z, 2)] = qsend[k]

        send_phase(1, i)

        @pl.when(i == 0)
        def _():
            for pair in others:
                wout_send(*pair).start()

    def order(t):
        return rem(z + (1 - 2 * rem(t, 2)) * div(t + 1, 2) + NZ, NZ)

    def group_row(k):
        return 2 * k + rem(k + c, 2)

    def q_here(k):
        return (group_row(k) == z) & (row_core == c)

    def kv_wait(s, p, half=0, size=TOK):
        start = half * HALF if size == HALF else 0
        ref = piece(s, p, start, size)
        remote(ref, ref, b_sem.at[0], kv_sem.at[s, p, half], at(c_=1 - c)).wait_recv()

    def hop(s, slot):
        p, device, half = (
            (y, at(y_=yp), None), (y, at(y_=ym), None), (y, at(c_=1 - c), None),
            (ym, at(y_=yp), 0), (ym, at(c_=1 - c), None),
            (yp, at(y_=ym), 1), (yp, at(c_=1 - c), None),
            (y2, at(c_=1 - c), None),
        )[slot]
        start, size = (0, TOK) if half is None else (half * HALF, HALF)
        ref = piece(s, p, start, size)
        return remote(ref, ref, b_sem.at[0], kv_sem.at[s, p, half or 0], device)

    def relay(t, k):
        @pl.when((k == 0) & (t < NZ))
        def _():
            s = order(t)

            @pl.when(rem(s, 2) == c)
            def _():
                @pl.when(jnp.logical_not((t == 0) & (row_core == c)))
                def _():
                    with jax.named_scope("wait_z"):
                        kv_wait(s, y)

                for slot in range(3):
                    hop(s, slot).start()

        @pl.when((k == 1) & (t >= 1) & (t < NZ + 1))
        def _():
            s = order(t - 1)

            @pl.when(rem(s, 2) == c)
            def _():
                with jax.named_scope("wait_ym"):
                    kv_wait(s, ym)
                hop(s, 3).start()
                hop(s, 4).start()

        @pl.when((k == 2) & (t >= 1) & (t < NZ + 1))
        def _():
            s = order(t - 1)

            @pl.when(rem(s, 2) == c)
            def _():
                with jax.named_scope("wait_yp"):
                    kv_wait(s, yp)
                hop(s, 5).start()
                hop(s, 6).start()

        @pl.when((k == 3) & (t >= 2) & (t < NZ + 2))
        def _():
            s = order(t - 2)

            @pl.when(rem(s, 2) == c)
            def _():
                with jax.named_scope("wait_y2"):
                    kv_wait(s, y2, 0, HALF)
                    kv_wait(s, y2, 1, HALF)
                hop(s, 7).start()

        @pl.when((k == 0) & (t >= 3))
        def _():
            s = order(t - 3)

            @pl.when(rem(s, 2) != c)
            def _():
                with jax.named_scope("wait_core"):
                    for p in range(NY):
                        kv_wait(s, jnp.int32(p))

    def tile(k, s):
        group = group_row(k) * NY + y
        lane = lax.broadcasted_iota(jnp.int32, (1, TOK), 1)
        parts = []
        for p in range(NY):
            key_group = s * NY + p
            limit = jnp.where(mask_ref[group, key_group] == 1, len_ref[key_group], 0)
            parts.append(jnp.where(lane < limit, 0.0, NEG).astype(jnp.float32))
        bias = jnp.concatenate(parts, axis=1)
        score = lax.dot_general(
            q[k], kv[s, :, 0:HS], (((1,), (1,)), ((), ())), preferred_element_type=jnp.float32
        ) + bias
        old = mx[k]
        new = jnp.maximum(old, jnp.max(score, axis=-1, keepdims=True))
        keep = jnp.exp2(old - new)
        weight = jnp.exp2(score - new[:, 0:1])
        mx[k] = new
        total = weight[:, 0:HS]
        for i in range(1, NY * TOK // HS):
            total += weight[:, i * HS:(i + 1) * HS]
        sm[k] = sm[k] * keep + total
        acc[k] = acc[k] * keep + jnp.dot(
            weight.astype(jnp.bfloat16), kv[s, :, HS:2 * HS], preferred_element_type=jnp.float32
        )

    def att_piece(x, u, half=None):
        start, size = (0, TOK) if half is None else (half * HALF, HALF)
        return att.at[x, pl.ds(start, size), pl.ds(pl.multiple_of(u * HS, HS), HS)]

    def att_remote(k):
        return remote(
            attsend.at[k], att_piece(m, row_u), c_sem.at[k], att_sem.at[m, row_u, 0],
            at(z_=group_row(k), c_=row_core),
        )

    def compute(j, k):
        row = group_row(k)
        away = rem(row - z + NZ, NZ)
        rank = jnp.where(away <= 3, 2 * away, jnp.where(away == 4, NZ - 1, 2 * (NZ - away) - 1))
        begin = jnp.maximum(rank - 2, 0)
        last = begin
        for i in range(NZ):
            last = jnp.where((order(jnp.int32(i)) <= row) & (i > last), i, last)

        @pl.when((j == begin) & jnp.logical_not(q_here(k)))
        def _():
            with jax.named_scope("wait_q"):
                remote(q.at[k], q.at[k], c_sem.at[k], q_sem.at[k], at(c_=1 - c)).wait_recv()

        @pl.when(j >= begin)
        def _():
            @pl.loop(jnp.where(j == begin, 0, j), j + 1)
            def _(i):
                s = order(i)

                @pl.when(s <= row)
                def _():
                    with jax.named_scope("tile"):
                        tile(k, s)

        @pl.when(j == last)
        def _():
            done = (acc[k] / jnp.sum(sm[k], axis=-1, keepdims=True)).astype(jnp.bfloat16)

            @pl.when(q_here(k))
            def _():
                att[m, :, pl.ds(pl.multiple_of(row_u * HS, HS), HS)] = done

            @pl.when(jnp.logical_not(q_here(k)))
            def _():
                attsend[k] = done
                att_remote(k).start()

    @pl.when(active)
    def _():
        @pl.loop(0, NZ + 3)
        def _(t):
            @pl.loop(0, 4)
            def _(k):
                relay(t, k)

                @pl.when((t == 0) & (k == 0))
                def _():
                    pl.delay(PAUSE)
                    send_rest(2)

                @pl.when((t == 2) & (k == 2))
                def _():
                    send_rest(3)

                @pl.when((t == 3) & (k == 1))
                def _():
                    send_rest(4)

                @pl.when(t >= 3)
                def _():
                    compute(t - 3, k)

    @pl.when(jnp.logical_not(active))
    def _():
        pl.delay(PAUSE)
        send_rest(2)
        pl.delay(2 * PAUSE)
        send_rest(3)

    def att_wait(x, u, half=None):
        ref = att_piece(x, u, half)
        remote(ref, ref, x_sem.at[0], att_sem.at[x, u, half or 0], at(c_=1 - c)).wait_recv()

    def att_hop(k, slot):
        u = 3 * c + k
        x, device, half = (
            (m, at(m_=xp), None), (m, at(m_=xm), None), (m, at(c_=1 - c), None),
            (xm, at(m_=xp), 0), (xm, at(c_=1 - c), None),
            (xp, at(m_=xm), 1), (xp, at(c_=1 - c), None),
            (x2, at(c_=1 - c), None),
        )[slot]
        ref = att_piece(x, u, half)
        return remote(ref, ref, x_sem.at[0], att_sem.at[x, u, half or 0], device)

    def project(x, core):
        cols = pl.ds(pl.multiple_of(core * width, HS), width)
        with jax.named_scope("project"):
            return jnp.dot(att[x, :, cols], wcol[x, cols, :], preferred_element_type=jnp.float32)

    @pl.loop(0, 3)
    def _(k):
        @pl.when(jnp.logical_not(q_local(k)))
        def _():
            with jax.named_scope("wait_att"):
                att_wait(m, 3 * c + k)

        for slot in range(3):
            att_hop(k, slot).start()

    with jax.named_scope("wait_wout"):
        wout_copy.wait()
        for pair in others:
            wout_send(*pair).wait_recv()
    branch[...] = project(m, c)

    @pl.loop(0, 3)
    def _(k):
        with jax.named_scope("wait_xm"):
            att_wait(xm, 3 * c + k)
        for slot in (3, 4):
            att_hop(k, slot).start()
        with jax.named_scope("wait_xp"):
            att_wait(xp, 3 * c + k)
        for slot in (5, 6):
            att_hop(k, slot).start()

    def project_across(x):
        with jax.named_scope("wait_across"):
            for k in range(3):
                att_wait(x, 3 * (1 - c) + k)
        branch[...] += project(x, 1 - c)

    project_across(m)
    branch[...] += project(xm, c)
    branch[...] += project(xp, c)

    @pl.loop(0, 3)
    def _(k):
        with jax.named_scope("wait_x2"):
            att_wait(x2, 3 * c + k, 0)
            att_wait(x2, 3 * c + k, 1)
        att_hop(k, 7).start()

    project_across(xm)
    project_across(xp)
    branch[...] += project(x2, c)
    project_across(x2)

    with jax.named_scope("final"):
        wide = lat[:, own_cols].astype(jnp.float32)
        out_ref[...] = (wide + mod[2, :, own_cols] * branch[...]).astype(jnp.bfloat16)

    def all_left(ref, sem):
        remote(ref, ref, sem, wor_sem.at[0, 0], at(c_=1 - c)).wait_send()

    with jax.named_scope("leave"):
        all_left(wqkv.at[0, pl.ds(0, 7 * width), pl.ds(0, width)], wos_sem.at[0])
        all_left(adapted.at[:, pl.ds(0, 21 * HS)], x_sem.at[0])

    @pl.loop(0, 3)
    def _(k):
        @pl.when(jnp.logical_not(kv_local(k)))
        def _():
            kv_remote(k).wait_send()

        @pl.when(jnp.logical_not(q_local(k)))
        def _():
            q_remote(k).wait_send()

    @pl.when(active)
    def _():
        all_left(kv.at[pl.ds(0, 7)], b_sem.at[0])

        @pl.loop(0, 4)
        def _(k):
            @pl.when(jnp.logical_not(q_here(k)))
            def _():
                att_remote(k).wait_send()


def shards(latents, modulation, w_qkv, w_out, block_mask, lengths):
    tok, d = latents.shape
    width = w_out.shape[0]
    dma = pltpu.SemaphoreType.DMA
    vmem = pltpu.VMEM
    bf16, f32 = jnp.bfloat16, jnp.float32
    anywhere = pl.BlockSpec(memory_space=pl.ANY)
    scalars = pl.BlockSpec(memory_space=pltpu.SMEM)
    return pl.pallas_call(
        kernel,
        out_shape=jax.ShapeDtypeStruct((tok, width), bf16),
        in_specs=[anywhere] * 4 + [scalars] * 2,
        out_specs=pl.BlockSpec(memory_space=pltpu.VMEM),
        scratch_shapes=[
            vmem((tok, d), bf16), vmem((3, 1, d), f32), vmem((tok, d), bf16),
            vmem((3, d, 3 * HS), bf16), vmem((3, tok, 2 * HS), bf16), vmem((3, tok, HS), bf16),
            vmem((NZ, NY * tok, 2 * HS), bf16), vmem((4, tok, HS), bf16),
            vmem((4, tok, HS), f32), vmem((4, tok, HS), f32), vmem((4, tok, HS), f32),
            vmem((4, tok, HS), bf16), vmem((NX, tok, 6 * HS), bf16), vmem((NX, 2 * width, width), bf16),
            vmem((tok, width), f32),
            dma((3,)), dma((3, 3)), dma((3,)), dma((3,)), dma((NZ, NY, 2)), dma((4,)),
            dma((1,)), dma((4,)), dma((NX, 6, 2)), dma((1,)), dma((1,)), dma((NX, 2)),
        ],
        compiler_params=pltpu.CompilerParams(
            collective_id=0, has_side_effects=True, vmem_limit_bytes=60 * 1024 * 1024
        ),
        name="attention_sublayer",
    )(latents, jnp.transpose(modulation, (1, 0, 2)), w_qkv, w_out, block_mask, lengths)


def solution(mesh):
    return jax.shard_map(
        shards,
        mesh=mesh,
        in_specs=(
            P("tm", None),
            P("tm", None, None),
            P(None, None, ("mp", "dec")),
            P(("mp", "dec"), None),
            P(),
            P(),
        ),
        out_specs=P("tm", ("mp", "dec")),
        check_vma=False,
    )
```

```python
import jax
import jax.numpy as jnp
from jax import lax
from jax.experimental import pallas as pl
from jax.experimental.pallas import tpu as pltpu
from jax.sharding import PartitionSpec as P

HS = 128
TOK = 256
NZ, NY, NX = 8, 4, 4
NEG = -1e30
LOG2E = 1.4426950408889634
HALF = TOK // 2
PAUSE = 2500


def rem(a, b):
    return lax.rem(a, jnp.int32(b))


def div(a, b):
    return lax.div(a, jnp.int32(b))


def kernel(
    lat_hbm, mod_hbm, wqkv_hbm, wout_hbm, mask_ref, len_ref, out_ref,
    lat, mod, adapted, wqkv, kvsend, qsend, kv, q, acc, mx, sm, attsend, att, wcol, branch,
    in_sem, w_sem, kvs_sem, qs_sem, kv_sem, q_sem, b_sem, c_sem, att_sem, x_sem, wos_sem, wor_sem,
):
    t_id = lax.axis_index("tm")
    z, y = div(t_id, NY), rem(t_id, NY)
    m = lax.axis_index("mp")
    c = lax.axis_index("dec")
    yp, ym, y2 = rem(y + 1, NY), rem(y + NY - 1, NY), rem(y + 2, NY)
    xp, xm, x2 = rem(m + 1, NX), rem(m + NX - 1, NX), rem(m + 2, NX)
    width = wout_hbm.shape[0]
    row_core = div(z, 4)
    row_u = 3 * row_core + rem(z, 4)
    active = rem(z, 4) != 3
    q_core = rem(div(z + 1, 2), 2)
    slab_core = rem(z, 2)

    rel = rem(z - 4 * c + NZ, NZ)
    first = jnp.where(rel == 1, 1, jnp.where((rel >= 2) & (rel <= 4), 2, 0))
    second = jnp.where(rel == 1, 0, jnp.where(rel == 5, 2, 1))

    def nearest(i):
        return jnp.where(i == 0, first, jnp.where(i == 1, second, 3 - first - second))

    def at(z_=z, y_=y, m_=m, c_=c):
        return {"tm": z_ * NY + y_, "mp": m_, "dec": c_}

    def remote(src, dst, ssem, rsem, device):
        return pltpu.make_async_remote_copy(
            src_ref=src, dst_ref=dst, send_sem=ssem, recv_sem=rsem,
            device_id=device, device_id_type=pl.DeviceIdType.MESH,
        )

    lat_copy = pltpu.make_async_copy(lat_hbm, lat, in_sem.at[0])
    mod_copy = pltpu.make_async_copy(mod_hbm, mod, in_sem.at[1])
    lat_copy.start()
    mod_copy.start()

    barrier = pltpu.get_barrier_semaphore()
    partners = [at(c_=1 - c), at(y_=yp), at(y_=ym)]
    for dz in range(1, NZ):
        for cc in range(2):
            partners.append(at(z_=rem(z + dz, NZ), c_=jnp.int32(cc)))
    for dx in range(1, NX):
        for cc in range(2):
            partners.append(at(m_=rem(m + dx, NX), c_=jnp.int32(cc)))
    for device in partners:
        pl.semaphore_signal(barrier, inc=1, device_id=device, device_id_type=pl.DeviceIdType.MESH)

    def weight_copy(k, part):
        cols = pl.ds(pl.multiple_of(k * HS, HS), HS)
        return pltpu.make_async_copy(
            wqkv_hbm.at[(part + 1) % 3, :, cols], wqkv.at[k, :, pl.ds(part * HS, HS)], w_sem.at[k, part]
        )

    for i in range(3):
        for part in range(3):
            weight_copy(nearest(i), part).start()
    own_cols = pl.ds(pl.multiple_of((2 * m + c) * width, HS), width)
    own_rows = pl.ds(pl.multiple_of(c * width, HS), width)
    wout_copy = pltpu.make_async_copy(wout_hbm.at[:, own_cols], wcol.at[m, own_rows, :], in_sem.at[2])
    wout_copy.start()

    mx[...] = jnp.full(mx.shape, NEG, jnp.float32)
    sm[...] = jnp.zeros(sm.shape, jnp.float32)
    acc[...] = jnp.zeros(acc.shape, jnp.float32)

    with jax.named_scope("load"):
        lat_copy.wait()
        mod_copy.wait()
    rows = 16

    @pl.loop(0, TOK // rows, unroll=4)
    def _(r):
        block = pl.ds(pl.multiple_of(r * rows, rows), rows)
        wide = lat[block, :].astype(jnp.float32)
        centred = wide - jnp.mean(wide, axis=-1, keepdims=True)
        var = jnp.mean(centred * centred, axis=-1, keepdims=True)
        normed = centred * lax.rsqrt(var + 1e-06)
        adapted[block, :] = (normed * (1.0 + mod[1]) + mod[0]).astype(jnp.bfloat16)

    with jax.named_scope("entry"):
        pl.semaphore_wait(barrier, len(partners))

    def wout_send(dx, dc):
        m_, c_ = rem(m + dx, NX), rem(c + dc, 2)
        cols = pl.ds(pl.multiple_of((2 * m_ + c_) * width, HS), width)
        return remote(
            wout_hbm.at[:, cols], wcol.at[m, own_rows, :],
            wos_sem.at[0], wor_sem.at[dx, dc], at(m_=m_, c_=c_),
        )

    others = [(dx, dc) for dx in range(NX) for dc in range(2) if (dx, dc) != (0, 0)]

    def piece(s, p, start=0, size=TOK):
        return kv.at[s, pl.ds(pl.multiple_of(p * TOK + start, HALF), size), :]

    def kv_remote(k):
        return remote(kvsend.at[k], piece(z, y), kvs_sem.at[k], kv_sem.at[z, y, 0], at(z_=4 * c + k, c_=slab_core))

    def q_remote(k):
        return remote(qsend.at[k], q.at[div(z, 2)], qs_sem.at[k], q_sem.at[div(z, 2)], at(z_=4 * c + k, c_=q_core))

    def kv_local(k):
        return (4 * c + k == z) & (slab_core == c)

    def q_local(k):
        return (4 * c + k == z) & (q_core == c)

    def send_phase(phase, i):
        k = nearest(i)
        away = rem(4 * c + k - z + NZ, NZ)
        far = jnp.maximum(jnp.minimum(away, NZ - away), 1)

        @pl.when((far == phase) & jnp.logical_not(kv_local(k)))
        def _():
            kv_remote(k).start()

        @pl.when((jnp.maximum(far - 1, 1) == phase) & jnp.logical_not(q_local(k)))
        def _():
            q_remote(k).start()

    def send_rest(phase):
        @pl.loop(0, 3)
        def _(i):
            send_phase(phase, i)

    @pl.loop(0, 3)
    def _(i):
        k = nearest(i)
        with jax.named_scope("weights"):
            for part in range(3):
                weight_copy(k, part).wait()
        made = jnp.dot(adapted[...], wqkv[k], preferred_element_type=jnp.float32)
        kvsend[k] = made[:, 0:2 * HS].astype(jnp.bfloat16)
        qsend[k] = (made[:, 2 * HS:3 * HS] * (LOG2E / HS**0.5)).astype(jnp.bfloat16)

        @pl.when(kv_local(k))
        def _():
            kv[z, pl.ds(pl.multiple_of(y * TOK, TOK), TOK), :] = kvsend[k]

        @pl.when(q_local(k))
        def _():
            q[div(z, 2)] = qsend[k]

        send_phase(1, i)

        @pl.when(i == 0)
        def _():
            for pair in others:
                wout_send(*pair).start()

    def order(t):
        return rem(z + (1 - 2 * rem(t, 2)) * div(t + 1, 2) + NZ, NZ)

    def group_row(k):
        return 2 * k + rem(k + c, 2)

    def q_here(k):
        return (group_row(k) == z) & (row_core == c)

    def kv_wait(s, p, half=0, size=TOK):
        start = half * HALF if size == HALF else 0
        ref = piece(s, p, start, size)
        remote(ref, ref, b_sem.at[0], kv_sem.at[s, p, half], at(c_=1 - c)).wait_recv()

    def hop(s, slot):
        p, device, half = (
            (y, at(y_=yp), None), (y, at(y_=ym), None), (y, at(c_=1 - c), None),
            (ym, at(y_=yp), 0), (ym, at(c_=1 - c), None),
            (yp, at(y_=ym), 1), (yp, at(c_=1 - c), None),
            (y2, at(c_=1 - c), None),
        )[slot]
        start, size = (0, TOK) if half is None else (half * HALF, HALF)
        ref = piece(s, p, start, size)
        return remote(ref, ref, b_sem.at[0], kv_sem.at[s, p, half or 0], device)

    def relay(t, k):
        @pl.when((k == 0) & (t < NZ))
        def _():
            s = order(t)

            @pl.when(rem(s, 2) == c)
            def _():
                @pl.when(jnp.logical_not((t == 0) & (row_core == c)))
                def _():
                    with jax.named_scope("wait_z"):
                        kv_wait(s, y)

                for slot in range(3):
                    hop(s, slot).start()

        @pl.when((k == 1) & (t >= 1) & (t < NZ + 1))
        def _():
            s = order(t - 1)

            @pl.when(rem(s, 2) == c)
            def _():
                with jax.named_scope("wait_ym"):
                    kv_wait(s, ym)
                hop(s, 3).start()
                hop(s, 4).start()

        @pl.when((k == 2) & (t >= 1) & (t < NZ + 1))
        def _():
            s = order(t - 1)

            @pl.when(rem(s, 2) == c)
            def _():
                with jax.named_scope("wait_yp"):
                    kv_wait(s, yp)
                hop(s, 5).start()
                hop(s, 6).start()

        @pl.when((k == 3) & (t >= 2) & (t < NZ + 2))
        def _():
            s = order(t - 2)

            @pl.when(rem(s, 2) == c)
            def _():
                with jax.named_scope("wait_y2"):
                    kv_wait(s, y2, 0, HALF)
                    kv_wait(s, y2, 1, HALF)
                hop(s, 7).start()

        @pl.when((k == 0) & (t >= 3))
        def _():
            s = order(t - 3)

            @pl.when(rem(s, 2) != c)
            def _():
                with jax.named_scope("wait_core"):
                    for p in range(NY):
                        kv_wait(s, jnp.int32(p))

    def tile(k, s):
        group = group_row(k) * NY + y
        lane = lax.broadcasted_iota(jnp.int32, (1, TOK), 1)
        parts = []
        for p in range(NY):
            key_group = s * NY + p
            limit = jnp.where(mask_ref[group, key_group] == 1, len_ref[key_group], 0)
            parts.append(jnp.where(lane < limit, 0.0, NEG).astype(jnp.float32))
        bias = jnp.concatenate(parts, axis=1)
        score = lax.dot_general(
            q[k], kv[s, :, 0:HS], (((1,), (1,)), ((), ())), preferred_element_type=jnp.float32
        ) + bias
        old = mx[k]
        new = jnp.maximum(old, jnp.max(score, axis=-1, keepdims=True))
        keep = jnp.exp2(old - new)
        weight = jnp.exp2(score - new[:, 0:1])
        mx[k] = new
        total = weight[:, 0:HS]
        for i in range(1, NY * TOK // HS):
            total += weight[:, i * HS:(i + 1) * HS]
        sm[k] = sm[k] * keep + total
        acc[k] = acc[k] * keep + jnp.dot(
            weight.astype(jnp.bfloat16), kv[s, :, HS:2 * HS], preferred_element_type=jnp.float32
        )

    def att_piece(x, u, half=None):
        start, size = (0, TOK) if half is None else (half * HALF, HALF)
        return att.at[x, pl.ds(start, size), pl.ds(pl.multiple_of(u * HS, HS), HS)]

    def att_remote(k):
        return remote(
            attsend.at[k], att_piece(m, row_u), c_sem.at[k], att_sem.at[m, row_u, 0],
            at(z_=group_row(k), c_=row_core),
        )

    def compute(j, k):
        row = group_row(k)
        away = rem(row - z + NZ, NZ)
        rank = jnp.where(away <= 3, 2 * away, jnp.where(away == 4, NZ - 1, 2 * (NZ - away) - 1))
        begin = jnp.maximum(rank - 2, 0)
        last = begin
        for i in range(NZ):
            last = jnp.where((order(jnp.int32(i)) <= row) & (i > last), i, last)

        @pl.when((j == begin) & jnp.logical_not(q_here(k)))
        def _():
            with jax.named_scope("wait_q"):
                remote(q.at[k], q.at[k], c_sem.at[k], q_sem.at[k], at(c_=1 - c)).wait_recv()

        @pl.when(j >= begin)
        def _():
            @pl.loop(jnp.where(j == begin, 0, j), j + 1)
            def _(i):
                s = order(i)

                @pl.when(s <= row)
                def _():
                    with jax.named_scope("tile"):
                        tile(k, s)

        @pl.when(j == last)
        def _():
            done = (acc[k] / jnp.sum(sm[k], axis=-1, keepdims=True)).astype(jnp.bfloat16)

            @pl.when(q_here(k))
            def _():
                att[m, :, pl.ds(pl.multiple_of(row_u * HS, HS), HS)] = done

            @pl.when(jnp.logical_not(q_here(k)))
            def _():
                attsend[k] = done
                att_remote(k).start()

    @pl.when(active)
    def _():
        @pl.loop(0, NZ + 3)
        def _(t):
            @pl.loop(0, 4)
            def _(k):
                relay(t, k)

                @pl.when((t == 0) & (k == 0))
                def _():
                    pl.delay(PAUSE)
                    send_rest(2)

                @pl.when((t == 3) & (k == 0))
                def _():
                    send_rest(3)

                @pl.when((t == 4) & (k == 1))
                def _():
                    send_rest(4)

                @pl.when(t >= 3)
                def _():
                    compute(t - 3, k)

    @pl.when(jnp.logical_not(active))
    def _():
        pl.delay(PAUSE)
        send_rest(2)
        pl.delay(5 * PAUSE // 2)
        send_rest(3)

    def att_wait(x, u, half=None):
        ref = att_piece(x, u, half)
        remote(ref, ref, x_sem.at[0], att_sem.at[x, u, half or 0], at(c_=1 - c)).wait_recv()

    def att_hop(k, slot):
        u = 3 * c + k
        x, device, half = (
            (m, at(m_=xp), None), (m, at(m_=xm), None), (m, at(c_=1 - c), None),
            (xm, at(m_=xp), 0), (xm, at(c_=1 - c), None),
            (xp, at(m_=xm), 1), (xp, at(c_=1 - c), None),
            (x2, at(c_=1 - c), None),
        )[slot]
        ref = att_piece(x, u, half)
        return remote(ref, ref, x_sem.at[0], att_sem.at[x, u, half or 0], device)

    def project(x, core):
        cols = pl.ds(pl.multiple_of(core * width, HS), width)
        with jax.named_scope("project"):
            return jnp.dot(att[x, :, cols], wcol[x, cols, :], preferred_element_type=jnp.float32)

    @pl.loop(0, 3)
    def _(k):
        @pl.when(jnp.logical_not(q_local(k)))
        def _():
            with jax.named_scope("wait_att"):
                att_wait(m, 3 * c + k)

        for slot in range(3):
            att_hop(k, slot).start()

    with jax.named_scope("wait_wout"):
        wout_copy.wait()
        for pair in others:
            wout_send(*pair).wait_recv()
    branch[...] = project(m, c)

    @pl.loop(0, 3)
    def _(k):
        with jax.named_scope("wait_xm"):
            att_wait(xm, 3 * c + k)
        for slot in (3, 4):
            att_hop(k, slot).start()
        with jax.named_scope("wait_xp"):
            att_wait(xp, 3 * c + k)
        for slot in (5, 6):
            att_hop(k, slot).start()

    def project_across(x):
        with jax.named_scope("wait_across"):
            for k in range(3):
                att_wait(x, 3 * (1 - c) + k)
        branch[...] += project(x, 1 - c)

    project_across(m)
    branch[...] += project(xm, c)
    branch[...] += project(xp, c)

    @pl.loop(0, 3)
    def _(k):
        with jax.named_scope("wait_x2"):
            att_wait(x2, 3 * c + k, 0)
            att_wait(x2, 3 * c + k, 1)
        att_hop(k, 7).start()

    project_across(xm)
    project_across(xp)
    branch[...] += project(x2, c)
    project_across(x2)

    with jax.named_scope("final"):
        wide = lat[:, own_cols].astype(jnp.float32)
        out_ref[...] = (wide + mod[2, :, own_cols] * branch[...]).astype(jnp.bfloat16)

    def all_left(ref, sem):
        remote(ref, ref, sem, wor_sem.at[0, 0], at(c_=1 - c)).wait_send()

    with jax.named_scope("leave"):
        all_left(wqkv.at[0, pl.ds(0, 7 * width), pl.ds(0, width)], wos_sem.at[0])
        all_left(adapted.at[:, pl.ds(0, 21 * HS)], x_sem.at[0])

    @pl.loop(0, 3)
    def _(k):
        @pl.when(jnp.logical_not(kv_local(k)))
        def _():
            kv_remote(k).wait_send()

        @pl.when(jnp.logical_not(q_local(k)))
        def _():
            q_remote(k).wait_send()

    @pl.when(active)
    def _():
        all_left(kv.at[pl.ds(0, 7)], b_sem.at[0])

        @pl.loop(0, 4)
        def _(k):
            @pl.when(jnp.logical_not(q_here(k)))
            def _():
                att_remote(k).wait_send()


def shards(latents, modulation, w_qkv, w_out, block_mask, lengths):
    tok, d = latents.shape
    width = w_out.shape[0]
    dma = pltpu.SemaphoreType.DMA
    vmem = pltpu.VMEM
    bf16, f32 = jnp.bfloat16, jnp.float32
    anywhere = pl.BlockSpec(memory_space=pl.ANY)
    scalars = pl.BlockSpec(memory_space=pltpu.SMEM)
    return pl.pallas_call(
        kernel,
        out_shape=pltpu.VMEM((tok, width), bf16),
        in_specs=[anywhere] * 4 + [scalars] * 2,
        out_specs=pl.BlockSpec(memory_space=pltpu.VMEM),
        scratch_shapes=[
            vmem((tok, d), bf16), vmem((3, 1, d), f32), vmem((tok, d), bf16),
            vmem((3, d, 3 * HS), bf16), vmem((3, tok, 2 * HS), bf16), vmem((3, tok, HS), bf16),
            vmem((NZ, NY * tok, 2 * HS), bf16), vmem((4, tok, HS), bf16),
            vmem((4, tok, HS), f32), vmem((4, tok, HS), f32), vmem((4, tok, HS), f32),
            vmem((4, tok, HS), bf16), vmem((NX, tok, 6 * HS), bf16), vmem((NX, 2 * width, width), bf16),
            vmem((tok, width), f32),
            dma((3,)), dma((3, 3)), dma((3,)), dma((3,)), dma((NZ, NY, 2)), dma((4,)),
            dma((1,)), dma((4,)), dma((NX, 6, 2)), dma((1,)), dma((1,)), dma((NX, 2)),
        ],
        compiler_params=pltpu.CompilerParams(
            collective_id=0, has_side_effects=True, vmem_limit_bytes=60 * 1024 * 1024
        ),
        name="attention_sublayer",
    )(latents, jnp.transpose(modulation, (1, 0, 2)), w_qkv, w_out, block_mask, lengths)


def solution(mesh):
    return jax.shard_map(
        shards,
        mesh=mesh,
        in_specs=(
            P("tm", None),
            P("tm", None, None),
            P(None, None, ("mp", "dec")),
            P(("mp", "dec"), None),
            P(),
            P(),
        ),
        out_specs=P("tm", ("mp", "dec")),
        check_vma=False,
    )
```

```python
import jax
import jax.numpy as jnp
from jax import lax
from jax.experimental import pallas as pl
from jax.experimental.pallas import tpu as pltpu
from jax.sharding import PartitionSpec as P

HS = 128
TOK = 256
NZ, NY, NX = 8, 4, 4
NEG = -1e30
LOG2E = 1.4426950408889634
HALF = TOK // 2
PAUSE = 2500


def rem(a, b):
    return lax.rem(a, jnp.int32(b))


def wrap(a, b):
    return jnp.where(a >= b, a - b, a)


def div(a, b):
    return lax.div(a, jnp.int32(b))


def kernel(
    lat_hbm, mod_hbm, wqkv_hbm, wout_hbm, mask_ref, len_ref, out_ref,
    lat, mod, adapted, wqkv, kvsend, qsend, kv, q, acc, mx, sm, attsend, att, wcol, branch,
    in_sem, w_sem, kvs_sem, qs_sem, kv_sem, q_sem, b_sem, c_sem, att_sem, x_sem, wos_sem, wor_sem,
):
    t_id = lax.axis_index("tm")
    z, y = div(t_id, NY), rem(t_id, NY)
    m = lax.axis_index("mp")
    c = lax.axis_index("dec")
    yp, ym, y2 = wrap(y + 1, NY), wrap(y + NY - 1, NY), wrap(y + 2, NY)
    xp, xm, x2 = wrap(m + 1, NX), wrap(m + NX - 1, NX), wrap(m + 2, NX)
    width = wout_hbm.shape[0]
    row_core = div(z, 4)
    row_u = 3 * row_core + rem(z, 4)
    active = rem(z, 4) != 3
    q_core = rem(div(z + 1, 2), 2)
    slab_core = rem(z, 2)

    rel = wrap(z - 4 * c + NZ, NZ)
    first = jnp.where(rel == 1, 1, jnp.where((rel >= 2) & (rel <= 4), 2, 0))
    second = jnp.where(rel == 1, 0, jnp.where(rel == 5, 2, 1))

    def nearest(i):
        return jnp.where(i == 0, first, jnp.where(i == 1, second, 3 - first - second))

    def at(z_=z, y_=y, m_=m, c_=c):
        return {"tm": z_ * NY + y_, "mp": m_, "dec": c_}

    def remote(src, dst, ssem, rsem, device):
        return pltpu.make_async_remote_copy(
            src_ref=src, dst_ref=dst, send_sem=ssem, recv_sem=rsem,
            device_id=device, device_id_type=pl.DeviceIdType.MESH,
        )

    lat_copy = pltpu.make_async_copy(lat_hbm, lat, in_sem.at[0])
    mod_copy = pltpu.make_async_copy(mod_hbm, mod, in_sem.at[1])
    lat_copy.start()
    mod_copy.start()

    barrier = pltpu.get_barrier_semaphore()
    partners = [at(c_=1 - c), at(y_=yp), at(y_=ym)]
    for dz in range(1, NZ):
        for cc in range(2):
            partners.append(at(z_=wrap(z + dz, NZ), c_=jnp.int32(cc)))
    for dx in range(1, NX):
        for cc in range(2):
            partners.append(at(m_=wrap(m + dx, NX), c_=jnp.int32(cc)))
    for device in partners:
        pl.semaphore_signal(barrier, inc=1, device_id=device, device_id_type=pl.DeviceIdType.MESH)

    def weight_copy(k, part):
        cols = pl.ds(pl.multiple_of(k * HS, HS), HS)
        return pltpu.make_async_copy(
            wqkv_hbm.at[(part + 1) % 3, :, cols], wqkv.at[k, :, pl.ds(part * HS, HS)], w_sem.at[k, part]
        )

    for i in range(3):
        for part in range(3):
            weight_copy(nearest(i), part).start()
    own_cols = pl.ds(pl.multiple_of((2 * m + c) * width, HS), width)
    own_rows = pl.ds(pl.multiple_of(c * width, HS), width)
    wout_copy = pltpu.make_async_copy(wout_hbm.at[:, own_cols], wcol.at[m, own_rows, :], in_sem.at[2])
    wout_copy.start()

    mx[...] = jnp.full(mx.shape, NEG, jnp.float32)
    sm[...] = jnp.zeros(sm.shape, jnp.float32)
    acc[...] = jnp.zeros(acc.shape, jnp.float32)

    with jax.named_scope("load"):
        lat_copy.wait()
        mod_copy.wait()
    rows = 16

    @pl.loop(0, TOK // rows, unroll=4)
    def _(r):
        block = pl.ds(pl.multiple_of(r * rows, rows), rows)
        wide = lat[block, :].astype(jnp.float32)
        centred = wide - jnp.mean(wide, axis=-1, keepdims=True)
        var = jnp.mean(centred * centred, axis=-1, keepdims=True)
        normed = centred * lax.rsqrt(var + 1e-06)
        adapted[block, :] = (normed * (1.0 + mod[1]) + mod[0]).astype(jnp.bfloat16)

    with jax.named_scope("entry"):
        pl.semaphore_wait(barrier, len(partners))

    def wout_send(dx, dc):
        m_, c_ = wrap(m + dx, NX), (1 - c if dc else c)
        cols = pl.ds(pl.multiple_of((2 * m_ + c_) * width, HS), width)
        return remote(
            wout_hbm.at[:, cols], wcol.at[m, own_rows, :],
            wos_sem.at[0], wor_sem.at[dx, dc], at(m_=m_, c_=c_),
        )

    others = [(dx, dc) for dx in range(NX) for dc in range(2) if (dx, dc) != (0, 0)]

    def piece(s, p, start=0, size=TOK):
        return kv.at[s, pl.ds(pl.multiple_of(p * TOK + start, HALF), size), :]

    def kv_remote(k):
        return remote(kvsend.at[k], piece(z, y), kvs_sem.at[k], kv_sem.at[z, y, 0], at(z_=4 * c + k, c_=slab_core))

    def q_remote(k):
        return remote(qsend.at[k], q.at[div(z, 2)], qs_sem.at[k], q_sem.at[div(z, 2)], at(z_=4 * c + k, c_=q_core))

    def kv_local(k):
        return (4 * c + k == z) & (slab_core == c)

    def q_local(k):
        return (4 * c + k == z) & (q_core == c)

    def send_phase(phase, i):
        k = nearest(i)
        away = wrap(4 * c + k - z + NZ, NZ)
        far = jnp.maximum(jnp.minimum(away, NZ - away), 1)

        @pl.when((far == phase) & jnp.logical_not(kv_local(k)))
        def _():
            kv_remote(k).start()

        @pl.when((jnp.maximum(far - 1, 1) == phase) & jnp.logical_not(q_local(k)))
        def _():
            q_remote(k).start()

    def send_rest(phase):
        @pl.loop(0, 3)
        def _(i):
            send_phase(phase, i)

    @pl.loop(0, 3)
    def _(i):
        k = nearest(i)
        with jax.named_scope("weights"):
            for part in range(3):
                weight_copy(k, part).wait()
        made = jnp.dot(adapted[...], wqkv[k], preferred_element_type=jnp.float32)
        kvsend[k] = made[:, 0:2 * HS].astype(jnp.bfloat16)
        qsend[k] = (made[:, 2 * HS:3 * HS] * (LOG2E / HS**0.5)).astype(jnp.bfloat16)

        @pl.when(kv_local(k))
        def _():
            kv[z, pl.ds(pl.multiple_of(y * TOK, TOK), TOK), :] = kvsend[k]

        @pl.when(q_local(k))
        def _():
            q[div(z, 2)] = qsend[k]

        send_phase(1, i)

        @pl.when(i == 0)
        def _():
            for pair in others:
                wout_send(*pair).start()

    def order(t):
        return wrap(z + jnp.where(rem(t, 2) == 1, NZ - div(t + 1, 2), div(t + 1, 2)), NZ)

    def group_row(k):
        return 2 * k + (1 - c if k % 2 else c)

    def q_here(k):
        return (group_row(k) == z) & (row_core == c)

    def kv_wait(s, p, half=0, size=TOK):
        start = half * HALF if size == HALF else 0
        ref = piece(s, p, start, size)
        remote(ref, ref, b_sem.at[0], kv_sem.at[s, p, half], at(c_=1 - c)).wait_recv()

    def hop(s, slot):
        p, device, half = (
            (y, at(y_=yp), None), (y, at(y_=ym), None), (y, at(c_=1 - c), None),
            (ym, at(y_=yp), 0), (ym, at(c_=1 - c), None),
            (yp, at(y_=ym), 1), (yp, at(c_=1 - c), None),
            (y2, at(c_=1 - c), None),
        )[slot]
        start, size = (0, TOK) if half is None else (half * HALF, HALF)
        ref = piece(s, p, start, size)
        return remote(ref, ref, b_sem.at[0], kv_sem.at[s, p, half or 0], device)

    def relay(t, k, rows, mine):
        if k == 0:
            @pl.when((t < NZ) & mine[0])
            def _():
                s = rows[0]

                @pl.when(jnp.logical_not((t == 0) & (row_core == c)))
                def _():
                    with jax.named_scope("wait_z"):
                        kv_wait(s, y)

                for slot in range(3):
                    hop(s, slot).start()

            @pl.when((t >= 3) & jnp.logical_not(mine[3]))
            def _():
                with jax.named_scope("wait_core"):
                    for p in range(NY):
                        kv_wait(rows[3], jnp.int32(p))

        if k == 1:
            @pl.when((t >= 1) & (t < NZ + 1) & mine[1])
            def _():
                with jax.named_scope("wait_ym"):
                    kv_wait(rows[1], ym)
                hop(rows[1], 3).start()
                hop(rows[1], 4).start()

        if k == 2:
            @pl.when((t >= 1) & (t < NZ + 1) & mine[1])
            def _():
                with jax.named_scope("wait_yp"):
                    kv_wait(rows[1], yp)
                hop(rows[1], 5).start()
                hop(rows[1], 6).start()

        if k == 3:
            @pl.when((t >= 2) & (t < NZ + 2) & mine[2])
            def _():
                with jax.named_scope("wait_y2"):
                    kv_wait(rows[2], y2, 0, HALF)
                    kv_wait(rows[2], y2, 1, HALF)
                hop(rows[2], 7).start()

    def tile(k, s):
        group = group_row(k) * NY + y
        lane = lax.broadcasted_iota(jnp.int32, (1, TOK), 1)
        parts = []
        for p in range(NY):
            key_group = s * NY + p
            limit = jnp.where(mask_ref[group, key_group] == 1, len_ref[key_group], 0)
            parts.append(jnp.where(lane < limit, 0.0, NEG).astype(jnp.float32))
        bias = jnp.concatenate(parts, axis=1)
        score = lax.dot_general(
            q[k], kv[s, :, 0:HS], (((1,), (1,)), ((), ())), preferred_element_type=jnp.float32
        ) + bias
        old = mx[k]
        new = jnp.maximum(old, jnp.max(score, axis=-1, keepdims=True))
        keep = jnp.exp2(old - new)
        weight = jnp.exp2(score - new[:, 0:1])
        mx[k] = new
        total = weight[:, 0:HS]
        for i in range(1, NY * TOK // HS):
            total += weight[:, i * HS:(i + 1) * HS]
        sm[k] = sm[k] * keep + total
        acc[k] = acc[k] * keep + jnp.dot(
            weight.astype(jnp.bfloat16), kv[s, :, HS:2 * HS], preferred_element_type=jnp.float32
        )

    def att_piece(x, u, half=None):
        start, size = (0, TOK) if half is None else (half * HALF, HALF)
        return att.at[x, pl.ds(start, size), pl.ds(pl.multiple_of(u * HS, HS), HS)]

    def att_remote(k):
        return remote(
            attsend.at[k], att_piece(m, row_u), c_sem.at[k], att_sem.at[m, row_u, 0],
            at(z_=group_row(k), c_=row_core),
        )

    def slot_steps(k, by_distance):
        row = group_row(k)
        away = wrap(row - z + NZ, NZ)
        rank = jnp.where(away <= 3, 2 * away, jnp.where(away == 4, NZ - 1, 2 * (NZ - away) - 1))
        begin = jnp.maximum(rank - 2, 0)
        last = begin
        for i, s in enumerate(by_distance):
            last = jnp.where((s <= row) & (i > last), i, last)
        return row, begin, last

    def compute(j, k, s_now, steps):
        row, begin, last = steps

        @pl.when((j == begin) & jnp.logical_not(q_here(k)))
        def _():
            with jax.named_scope("wait_q"):
                remote(q.at[k], q.at[k], c_sem.at[k], q_sem.at[k], at(c_=1 - c)).wait_recv()

        @pl.when(j >= begin)
        def _():
            @pl.loop(jnp.where(j == begin, 0, j), j + 1)
            def _(i):
                s = jnp.where(i == j, s_now, order(i))

                @pl.when(s <= row)
                def _():
                    with jax.named_scope("tile"):
                        tile(k, s)

        @pl.when(j == last)
        def _():
            done = (acc[k] / jnp.sum(sm[k], axis=-1, keepdims=True)).astype(jnp.bfloat16)

            @pl.when(q_here(k))
            def _():
                att[m, :, pl.ds(pl.multiple_of(row_u * HS, HS), HS)] = done

            @pl.when(jnp.logical_not(q_here(k)))
            def _():
                attsend[k] = done
                att_remote(k).start()

    @pl.when(active)
    def _():
        by_distance = [wrap(z + (NZ - (i + 1) // 2 if i % 2 else i // 2), NZ) for i in range(NZ)]
        steps = [slot_steps(k, by_distance) for k in range(4)]

        def step(t, earlier):
            rows = (order(t),) + earlier
            mine = [rem(s, 2) == c for s in rows]
            for k in range(4):
                relay(t, k, rows, mine)
                if k == 0:
                    @pl.when(t == 0)
                    def _():
                        pl.delay(PAUSE)
                        send_rest(2)

                    @pl.when(t == 3)
                    def _():
                        send_rest(3)

                if k == 1:
                    @pl.when(t == 4)
                    def _():
                        send_rest(4)

                @pl.when(t >= 3)
                def _():
                    compute(t - 3, k, rows[3], steps[k])

            return rows[:3]

        lax.fori_loop(0, NZ + 3, step, (z, z, z))

    @pl.when(jnp.logical_not(active))
    def _():
        pl.delay(PAUSE)
        send_rest(2)
        pl.delay(5 * PAUSE // 2)
        send_rest(3)

    def att_wait(x, u, half=None):
        ref = att_piece(x, u, half)
        remote(ref, ref, x_sem.at[0], att_sem.at[x, u, half or 0], at(c_=1 - c)).wait_recv()

    def att_hop(k, slot):
        u = 3 * c + k
        x, device, half = (
            (m, at(m_=xp), None), (m, at(m_=xm), None), (m, at(c_=1 - c), None),
            (xm, at(m_=xp), 0), (xm, at(c_=1 - c), None),
            (xp, at(m_=xm), 1), (xp, at(c_=1 - c), None),
            (x2, at(c_=1 - c), None),
        )[slot]
        ref = att_piece(x, u, half)
        return remote(ref, ref, x_sem.at[0], att_sem.at[x, u, half or 0], device)

    def project(x, core):
        cols = pl.ds(pl.multiple_of(core * width, HS), width)
        with jax.named_scope("project"):
            return jnp.dot(att[x, :, cols], wcol[x, cols, :], preferred_element_type=jnp.float32)

    @pl.loop(0, 3)
    def _(k):
        @pl.when(jnp.logical_not(q_local(k)))
        def _():
            with jax.named_scope("wait_att"):
                att_wait(m, 3 * c + k)

        for slot in range(3):
            att_hop(k, slot).start()

    with jax.named_scope("wait_wout"):
        wout_copy.wait()
        for pair in others:
            wout_send(*pair).wait_recv()
    branch[...] = project(m, c)

    @pl.loop(0, 3)
    def _(k):
        with jax.named_scope("wait_xm"):
            att_wait(xm, 3 * c + k)
        for slot in (3, 4):
            att_hop(k, slot).start()
        with jax.named_scope("wait_xp"):
            att_wait(xp, 3 * c + k)
        for slot in (5, 6):
            att_hop(k, slot).start()

    def project_across(x):
        with jax.named_scope("wait_across"):
            for k in range(3):
                att_wait(x, 3 * (1 - c) + k)
        branch[...] += project(x, 1 - c)

    project_across(m)
    branch[...] += project(xm, c)
    branch[...] += project(xp, c)

    @pl.loop(0, 3)
    def _(k):
        with jax.named_scope("wait_x2"):
            att_wait(x2, 3 * c + k, 0)
            att_wait(x2, 3 * c + k, 1)
        att_hop(k, 7).start()

    project_across(xm)
    project_across(xp)
    branch[...] += project(x2, c)
    project_across(x2)

    with jax.named_scope("final"):
        wide = lat[:, own_cols].astype(jnp.float32)
        out_ref[...] = (wide + mod[2, :, own_cols] * branch[...]).astype(jnp.bfloat16)

    def all_left(ref, sem):
        remote(ref, ref, sem, wor_sem.at[0, 0], at(c_=1 - c)).wait_send()

    with jax.named_scope("leave"):
        all_left(wqkv.at[0, pl.ds(0, 7 * width), pl.ds(0, width)], wos_sem.at[0])
        all_left(adapted.at[:, pl.ds(0, 21 * HS)], x_sem.at[0])

    @pl.loop(0, 3)
    def _(k):
        @pl.when(jnp.logical_not(kv_local(k)))
        def _():
            kv_remote(k).wait_send()

        @pl.when(jnp.logical_not(q_local(k)))
        def _():
            q_remote(k).wait_send()

    @pl.when(active)
    def _():
        all_left(kv.at[pl.ds(0, 7)], b_sem.at[0])

        for k in range(4):
            @pl.when(jnp.logical_not(q_here(k)))
            def _():
                att_remote(k).wait_send()


def shards(latents, modulation, w_qkv, w_out, block_mask, lengths):
    tok, d = latents.shape
    width = w_out.shape[0]
    dma = pltpu.SemaphoreType.DMA
    vmem = pltpu.VMEM
    bf16, f32 = jnp.bfloat16, jnp.float32
    anywhere = pl.BlockSpec(memory_space=pl.ANY)
    scalars = pl.BlockSpec(memory_space=pltpu.SMEM)
    return pl.pallas_call(
        kernel,
        out_shape=pltpu.VMEM((tok, width), bf16),
        in_specs=[anywhere] * 4 + [scalars] * 2,
        out_specs=pl.BlockSpec(memory_space=pltpu.VMEM),
        scratch_shapes=[
            vmem((tok, d), bf16), vmem((3, 1, d), f32), vmem((tok, d), bf16),
            vmem((3, d, 3 * HS), bf16), vmem((3, tok, 2 * HS), bf16), vmem((3, tok, HS), bf16),
            vmem((NZ, NY * tok, 2 * HS), bf16), vmem((4, tok, HS), bf16),
            vmem((4, tok, HS), f32), vmem((4, tok, HS), f32), vmem((4, tok, HS), f32),
            vmem((4, tok, HS), bf16), vmem((NX, tok, 6 * HS), bf16), vmem((NX, 2 * width, width), bf16),
            vmem((tok, width), f32),
            dma((3,)), dma((3, 3)), dma((3,)), dma((3,)), dma((NZ, NY, 2)), dma((4,)),
            dma((1,)), dma((4,)), dma((NX, 6, 2)), dma((1,)), dma((1,)), dma((NX, 2)),
        ],
        compiler_params=pltpu.CompilerParams(
            collective_id=0, has_side_effects=True, vmem_limit_bytes=60 * 1024 * 1024
        ),
        name="attention_sublayer",
    )(latents, jnp.transpose(modulation, (1, 0, 2)), w_qkv, w_out, block_mask, lengths)


def solution(mesh):
    return jax.shard_map(
        shards,
        mesh=mesh,
        in_specs=(
            P("tm", None),
            P("tm", None, None),
            P(None, None, ("mp", "dec")),
            P(("mp", "dec"), None),
            P(),
            P(),
        ),
        out_specs=P("tm", ("mp", "dec")),
        check_vma=False,
    )
```

```python
import jax
import jax.numpy as jnp
from jax import lax
from jax.experimental import pallas as pl
from jax.experimental.pallas import tpu as pltpu
from jax.sharding import PartitionSpec as P

HS = 128
TOK = 256
NZ, NY, NX = 8, 4, 4
NEG = -1e30
HALF = TOK // 2
PAUSE = 2500


def rem(a, b):
    return lax.rem(a, jnp.int32(b))


def wrap(a, b):
    return jnp.where(a >= b, a - b, a)


def div(a, b):
    return lax.div(a, jnp.int32(b))


def kernel(
    lat_hbm, mod_hbm, wqkv_hbm, wout_hbm, mask_ref, len_ref, out_ref,
    lat, mod, adapted, wqkv, kvsend, qsend, kv, q, acc, mx, sm, attsend, att, wcol, branch,
    in_sem, w_sem, kvs_sem, qs_sem, kv_sem, q_sem, b_sem, c_sem, att_sem, x_sem, wos_sem, wor_sem,
):
    t_id = lax.axis_index("tm")
    z, y = div(t_id, NY), rem(t_id, NY)
    m = lax.axis_index("mp")
    c = lax.axis_index("dec")
    yp, ym, y2 = wrap(y + 1, NY), wrap(y + NY - 1, NY), wrap(y + 2, NY)
    xp, xm, x2 = wrap(m + 1, NX), wrap(m + NX - 1, NX), wrap(m + 2, NX)
    width = wout_hbm.shape[0]
    row_core = div(z, 4)
    row_u = 3 * row_core + rem(z, 4)
    active = rem(z, 4) != 3
    q_core = rem(div(z + 1, 2), 2)
    slab_core = rem(z, 2)

    rel = wrap(z - 4 * c + NZ, NZ)
    first = jnp.where(rel == 1, 1, jnp.where((rel >= 2) & (rel <= 4), 2, 0))
    second = jnp.where(rel == 1, 0, jnp.where(rel == 5, 2, 1))

    def nearest(i):
        return jnp.where(i == 0, first, jnp.where(i == 1, second, 3 - first - second))

    def at(z_=z, y_=y, m_=m, c_=c):
        return {"tm": z_ * NY + y_, "mp": m_, "dec": c_}

    def remote(src, dst, ssem, rsem, device):
        return pltpu.make_async_remote_copy(
            src_ref=src, dst_ref=dst, send_sem=ssem, recv_sem=rsem,
            device_id=device, device_id_type=pl.DeviceIdType.MESH,
        )

    lat_copy = pltpu.make_async_copy(lat_hbm, lat, in_sem.at[0])
    mod_copy = pltpu.make_async_copy(mod_hbm, mod, in_sem.at[1])
    lat_copy.start()
    mod_copy.start()

    barrier = pltpu.get_barrier_semaphore()
    partners = [at(c_=1 - c), at(y_=yp), at(y_=ym)]
    for dz in range(1, NZ):
        for cc in range(2):
            partners.append(at(z_=wrap(z + dz, NZ), c_=jnp.int32(cc)))
    for dx in range(1, NX):
        for cc in range(2):
            partners.append(at(m_=wrap(m + dx, NX), c_=jnp.int32(cc)))
    for device in partners:
        pl.semaphore_signal(barrier, inc=1, device_id=device, device_id_type=pl.DeviceIdType.MESH)

    def weight_copy(k, part):
        cols = pl.ds(pl.multiple_of(k * HS, HS), HS)
        return pltpu.make_async_copy(
            wqkv_hbm.at[(part + 1) % 3, :, cols], wqkv.at[k, :, pl.ds(part * HS, HS)], w_sem.at[k, part]
        )

    for i in range(3):
        for part in range(3):
            weight_copy(nearest(i), part).start()
    own_cols = pl.ds(pl.multiple_of((2 * m + c) * width, HS), width)
    own_rows = pl.ds(pl.multiple_of(c * width, HS), width)
    wout_copy = pltpu.make_async_copy(wout_hbm.at[:, own_cols], wcol.at[m, own_rows, :], in_sem.at[2])
    wout_copy.start()

    mx[...] = jnp.full(mx.shape, NEG, jnp.float32)
    sm[...] = jnp.zeros(sm.shape, jnp.float32)
    acc[...] = jnp.zeros(acc.shape, jnp.float32)

    with jax.named_scope("load"):
        lat_copy.wait()
        mod_copy.wait()
    rows = 16

    @pl.loop(0, TOK // rows, unroll=4)
    def _(r):
        block = pl.ds(pl.multiple_of(r * rows, rows), rows)
        wide = lat[block, :].astype(jnp.float32)
        centred = wide - jnp.mean(wide, axis=-1, keepdims=True)
        var = jnp.mean(centred * centred, axis=-1, keepdims=True)
        normed = centred * lax.rsqrt(var + 1e-06)
        adapted[block, :] = (normed * (1.0 + mod[1]) + mod[0]).astype(jnp.bfloat16)

    with jax.named_scope("entry"):
        pl.semaphore_wait(barrier, len(partners))

    def wout_send(dx, dc):
        m_, c_ = wrap(m + dx, NX), (1 - c if dc else c)
        cols = pl.ds(pl.multiple_of((2 * m_ + c_) * width, HS), width)
        return remote(
            wout_hbm.at[:, cols], wcol.at[m, own_rows, :],
            wos_sem.at[0], wor_sem.at[dx, dc], at(m_=m_, c_=c_),
        )

    others = [(dx, dc) for dx in range(NX) for dc in range(2) if (dx, dc) != (0, 0)]

    def piece(s, p, start=0, size=TOK):
        return kv.at[s, pl.ds(pl.multiple_of(p * TOK + start, HALF), size), :]

    def kv_remote(k):
        return remote(kvsend.at[k], piece(z, y), kvs_sem.at[k], kv_sem.at[z, y, 0], at(z_=4 * c + k, c_=slab_core))

    def q_remote(k):
        return remote(qsend.at[k], q.at[div(z, 2)], qs_sem.at[k], q_sem.at[div(z, 2)], at(z_=4 * c + k, c_=q_core))

    def hop(s, slot):
        p, device, half = (
            (y, at(y_=yp), None), (y, at(y_=ym), None), (y, at(c_=1 - c), None),
            (ym, at(y_=yp), 0), (ym, at(c_=1 - c), None),
            (yp, at(y_=ym), 1), (yp, at(c_=1 - c), None),
            (y2, at(c_=1 - c), None),
        )[slot]
        start, size = (0, TOK) if half is None else (half * HALF, HALF)
        ref = piece(s, p, start, size)
        return remote(ref, ref, b_sem.at[0], kv_sem.at[s, p, half or 0], device)

    def kv_local(k):
        return (4 * c + k == z) & (slab_core == c)

    def q_local(k):
        return (4 * c + k == z) & (q_core == c)

    def send_phase(phase, i):
        k = nearest(i)
        away = wrap(4 * c + k - z + NZ, NZ)
        far = jnp.maximum(jnp.minimum(away, NZ - away), 1)

        @pl.when((far == phase) & jnp.logical_not(kv_local(k)))
        def _():
            kv_remote(k).start()

        @pl.when((jnp.maximum(far - 1, 1) == phase) & jnp.logical_not(q_local(k)))
        def _():
            q_remote(k).start()

    def send_rest(phase):
        @pl.loop(0, 3)
        def _(i):
            send_phase(phase, i)

    @pl.loop(0, 3)
    def _(i):
        k = nearest(i)
        with jax.named_scope("weights"):
            for part in range(3):
                weight_copy(k, part).wait()
        made = jnp.dot(adapted[...], wqkv[k], preferred_element_type=jnp.float32)
        kvsend[k] = made[:, 0:2 * HS].astype(jnp.bfloat16)
        qsend[k] = (made[:, 2 * HS:3 * HS] * (1.0 / HS**0.5)).astype(jnp.bfloat16)

        @pl.when(kv_local(k))
        def _():
            kv[z, pl.ds(pl.multiple_of(y * TOK, TOK), TOK), :] = kvsend[k]

        @pl.when(q_local(k))
        def _():
            q[div(z, 2)] = qsend[k]

        @pl.when((i == 0) & kv_local(k))
        def _():
            for slot in range(3):
                hop(z, slot).start()

        send_phase(1, i)

        @pl.when(i == 0)
        def _():
            for pair in others:
                wout_send(*pair).start()

    def order(t):
        return wrap(z + jnp.where(rem(t, 2) == 1, NZ - div(t + 1, 2), div(t + 1, 2)), NZ)

    def group_row(k):
        return 2 * k + (1 - c if k % 2 else c)

    def q_here(k):
        return (group_row(k) == z) & (row_core == c)

    def kv_wait(s, p, half=0, size=TOK):
        start = half * HALF if size == HALF else 0
        ref = piece(s, p, start, size)
        remote(ref, ref, b_sem.at[0], kv_sem.at[s, p, half], at(c_=1 - c)).wait_recv()

    def relay(t, k, rows, mine):
        if k == 0:
            @pl.when((t < NZ) & mine[0])
            def _():
                s = rows[0]

                @pl.when(jnp.logical_not((t == 0) & (row_core == c)))
                def _():
                    with jax.named_scope("wait_z"):
                        kv_wait(s, y)

                @pl.when(jnp.logical_not((t == 0) & (row_core == c)))
                def _():
                    for slot in range(3):
                        hop(s, slot).start()

            @pl.when((t >= 3) & jnp.logical_not(mine[3]))
            def _():
                with jax.named_scope("wait_core"):
                    for p in range(NY):
                        kv_wait(rows[3], jnp.int32(p))

        if k == 1:
            @pl.when((t >= 1) & (t < NZ + 1) & mine[1])
            def _():
                with jax.named_scope("wait_ym"):
                    kv_wait(rows[1], ym)
                hop(rows[1], 3).start()
                hop(rows[1], 4).start()

        if k == 2:
            @pl.when((t >= 1) & (t < NZ + 1) & mine[1])
            def _():
                with jax.named_scope("wait_yp"):
                    kv_wait(rows[1], yp)
                hop(rows[1], 5).start()
                hop(rows[1], 6).start()

        if k == 3:
            @pl.when((t >= 2) & (t < NZ + 2) & mine[2])
            def _():
                with jax.named_scope("wait_y2"):
                    kv_wait(rows[2], y2, 0, HALF)
                    kv_wait(rows[2], y2, 1, HALF)
                hop(rows[2], 7).start()

    def tile(k, s):
        group = group_row(k) * NY + y
        lane = lax.broadcasted_iota(jnp.int32, (1, TOK), 1)
        parts = []
        for p in range(NY):
            key_group = s * NY + p
            limit = jnp.where(mask_ref[group, key_group] == 1, len_ref[key_group], 0)
            parts.append(jnp.where(lane < limit, 0.0, NEG).astype(jnp.float32))
        bias = jnp.concatenate(parts, axis=1)
        score = lax.dot_general(
            q[k], kv[s, :, 0:HS], (((1,), (1,)), ((), ())), preferred_element_type=jnp.float32
        ) + bias
        old = mx[k]
        new = jnp.maximum(old, jnp.max(score, axis=-1, keepdims=True))
        keep = jnp.exp(old - new)
        weight = jnp.exp(score - new[:, 0:1])
        mx[k] = new
        total = weight[:, 0:HS]
        for i in range(1, NY * TOK // HS):
            total += weight[:, i * HS:(i + 1) * HS]
        sm[k] = sm[k] * keep + total
        acc[k] = acc[k] * keep + jnp.dot(
            weight.astype(jnp.bfloat16), kv[s, :, HS:2 * HS], preferred_element_type=jnp.float32
        )

    def att_piece(x, u, half=None):
        start, size = (0, TOK) if half is None else (half * HALF, HALF)
        return att.at[x, pl.ds(start, size), pl.ds(pl.multiple_of(u * HS, HS), HS)]

    def att_remote(k):
        return remote(
            attsend.at[k], att_piece(m, row_u), c_sem.at[k], att_sem.at[m, row_u, 0],
            at(z_=group_row(k), c_=row_core),
        )

    def slot_steps(k, by_distance):
        row = group_row(k)
        away = wrap(row - z + NZ, NZ)
        rank = jnp.where(away <= 3, 2 * away, jnp.where(away == 4, NZ - 1, 2 * (NZ - away) - 1))
        begin = jnp.maximum(rank - 2, 0)
        last = begin
        for i, s in enumerate(by_distance):
            last = jnp.where((s <= row) & (i > last), i, last)
        return row, begin, last

    def compute(j, k, s_now, steps):
        row, begin, last = steps

        @pl.when((j == begin) & jnp.logical_not(q_here(k)))
        def _():
            with jax.named_scope("wait_q"):
                remote(q.at[k], q.at[k], c_sem.at[k], q_sem.at[k], at(c_=1 - c)).wait_recv()

        @pl.when(j >= begin)
        def _():
            @pl.loop(jnp.where(j == begin, 0, j), j + 1)
            def _(i):
                s = jnp.where(i == j, s_now, order(i))

                @pl.when(s <= row)
                def _():
                    with jax.named_scope("tile"):
                        tile(k, s)

        @pl.when(j == last)
        def _():
            done = (acc[k] / jnp.sum(sm[k], axis=-1, keepdims=True)).astype(jnp.bfloat16)

            @pl.when(q_here(k))
            def _():
                att[m, :, pl.ds(pl.multiple_of(row_u * HS, HS), HS)] = done

            @pl.when(jnp.logical_not(q_here(k)))
            def _():
                attsend[k] = done
                att_remote(k).start()

    @pl.when(active)
    def _():
        by_distance = [wrap(z + (NZ - (i + 1) // 2 if i % 2 else i // 2), NZ) for i in range(NZ)]
        steps = [slot_steps(k, by_distance) for k in range(4)]

        def step(t, earlier):
            rows = (order(t),) + earlier
            mine = [rem(s, 2) == c for s in rows]
            for k in range(4):
                relay(t, k, rows, mine)
                if k == 0:
                    @pl.when(t == 0)
                    def _():
                        pl.delay(PAUSE)
                        send_rest(2)

                    @pl.when(t == 3)
                    def _():
                        send_rest(3)

                if k == 1:
                    @pl.when(t == 4)
                    def _():
                        send_rest(4)

                @pl.when(t >= 3)
                def _():
                    compute(t - 3, k, rows[3], steps[k])

            return rows[:3]

        lax.fori_loop(0, NZ + 3, step, (z, z, z))

    @pl.when(jnp.logical_not(active))
    def _():
        pl.delay(PAUSE)
        send_rest(2)
        pl.delay(5 * PAUSE // 2)
        send_rest(3)

    def att_wait(x, u, half=None):
        ref = att_piece(x, u, half)
        remote(ref, ref, x_sem.at[0], att_sem.at[x, u, half or 0], at(c_=1 - c)).wait_recv()

    def att_hop(k, slot):
        u = 3 * c + k
        x, device, half = (
            (m, at(m_=xp), None), (m, at(m_=xm), None), (m, at(c_=1 - c), None),
            (xm, at(m_=xp), 0), (xm, at(c_=1 - c), None),
            (xp, at(m_=xm), 1), (xp, at(c_=1 - c), None),
            (x2, at(c_=1 - c), None), (m, at(m_=x2), None),
        )[slot]
        ref = att_piece(x, u, half)
        return remote(ref, ref, x_sem.at[0], att_sem.at[x, u, half or 0], device)

    def project(x, core):
        cols = pl.ds(pl.multiple_of(core * width, HS), width)
        with jax.named_scope("project"):
            return jnp.dot(att[x, :, cols], wcol[x, cols, :], preferred_element_type=jnp.float32)

    @pl.loop(0, 3)
    def _(k):
        @pl.when(jnp.logical_not(q_local(k)))
        def _():
            with jax.named_scope("wait_att"):
                att_wait(m, 3 * c + k)

        @pl.when(k == 2)
        def _():
            att_hop(k, 8).start()

        for slot in range(3):
            att_hop(k, slot).start()

    with jax.named_scope("wait_wout"):
        wout_copy.wait()
        for pair in others:
            wout_send(*pair).wait_recv()
    branch[...] = project(m, c)

    @pl.loop(0, 3)
    def _(k):
        with jax.named_scope("wait_xm"):
            att_wait(xm, 3 * c + k)
        @pl.when(k < 2)
        def _():
            att_hop(k, 3).start()

        att_hop(k, 4).start()
        with jax.named_scope("wait_xp"):
            att_wait(xp, 3 * c + k)
        @pl.when(k < 2)
        def _():
            att_hop(k, 5).start()

        att_hop(k, 6).start()

    def project_across(x):
        with jax.named_scope("wait_across"):
            for k in range(3):
                att_wait(x, 3 * (1 - c) + k)
        branch[...] += project(x, 1 - c)

    project_across(m)
    branch[...] += project(xm, c)
    branch[...] += project(xp, c)

    @pl.loop(0, 3)
    def _(k):
        with jax.named_scope("wait_x2"):
            @pl.when(k < 2)
            def _():
                att_wait(x2, 3 * c + k, 0)
                att_wait(x2, 3 * c + k, 1)

            @pl.when(k == 2)
            def _():
                att_wait(x2, 3 * c + k)

        att_hop(k, 7).start()

    project_across(xm)
    project_across(xp)
    branch[...] += project(x2, c)
    project_across(x2)

    with jax.named_scope("final"):
        wide = lat[:, own_cols].astype(jnp.float32)
        out_ref[...] = (wide + mod[2, :, own_cols] * branch[...]).astype(jnp.bfloat16)

    def all_left(ref, sem):
        remote(ref, ref, sem, wor_sem.at[0, 0], at(c_=1 - c)).wait_send()

    with jax.named_scope("leave"):
        all_left(wqkv.at[0, pl.ds(0, 7 * width), pl.ds(0, width)], wos_sem.at[0])
        all_left(adapted.at[:, pl.ds(0, 21 * HS)], x_sem.at[0])

    @pl.loop(0, 3)
    def _(k):
        @pl.when(jnp.logical_not(kv_local(k)))
        def _():
            kv_remote(k).wait_send()

        @pl.when(jnp.logical_not(q_local(k)))
        def _():
            q_remote(k).wait_send()

    @pl.when(active)
    def _():
        all_left(kv.at[pl.ds(0, 7)], b_sem.at[0])

        for k in range(4):
            @pl.when(jnp.logical_not(q_here(k)))
            def _():
                att_remote(k).wait_send()


def shards(latents, modulation, w_qkv, w_out, block_mask, lengths):
    tok, d = latents.shape
    width = w_out.shape[0]
    dma = pltpu.SemaphoreType.DMA
    vmem = pltpu.VMEM
    bf16, f32 = jnp.bfloat16, jnp.float32
    anywhere = pl.BlockSpec(memory_space=pl.ANY)
    scalars = pl.BlockSpec(memory_space=pltpu.SMEM)
    return pl.pallas_call(
        kernel,
        out_shape=pltpu.VMEM((tok, width), bf16),
        in_specs=[anywhere] * 4 + [scalars] * 2,
        out_specs=pl.BlockSpec(memory_space=pltpu.VMEM),
        scratch_shapes=[
            vmem((tok, d), bf16), vmem((3, 1, d), f32), vmem((tok, d), bf16),
            vmem((3, d, 3 * HS), bf16), vmem((3, tok, 2 * HS), bf16), vmem((3, tok, HS), bf16),
            vmem((NZ, NY * tok, 2 * HS), bf16), vmem((4, tok, HS), bf16),
            vmem((4, tok, HS), f32), vmem((4, tok, HS), f32), vmem((4, tok, HS), f32),
            vmem((4, tok, HS), bf16), vmem((NX, tok, 6 * HS), bf16), vmem((NX, 2 * width, width), bf16),
            vmem((tok, width), f32),
            dma((3,)), dma((3, 3)), dma((3,)), dma((3,)), dma((NZ, NY, 2)), dma((4,)),
            dma((1,)), dma((4,)), dma((NX, 6, 2)), dma((1,)), dma((1,)), dma((NX, 2)),
        ],
        compiler_params=pltpu.CompilerParams(
            collective_id=0, has_side_effects=True, vmem_limit_bytes=60 * 1024 * 1024
        ),
        name="attention_sublayer",
    )(latents, jnp.transpose(modulation, (1, 0, 2)), w_qkv, w_out, block_mask, lengths)


def solution(mesh):
    return jax.shard_map(
        shards,
        mesh=mesh,
        in_specs=(
            P("tm", None),
            P("tm", None, None),
            P(None, None, ("mp", "dec")),
            P(("mp", "dec"), None),
            P(),
            P(),
        ),
        out_specs=P("tm", ("mp", "dec")),
        check_vma=False,
    )
```

```python
import jax
import jax.numpy as jnp
from jax import lax
from jax.experimental import pallas as pl
from jax.experimental.pallas import tpu as pltpu
from jax.sharding import PartitionSpec as P

HS = 128
TOK = 256
NZ, NY, NX = 8, 4, 4
NEG = -1e30
HALF = TOK // 2
PAUSE = 2500


def rem(a, b):
    return lax.rem(a, jnp.int32(b))


def wrap(a, b):
    return jnp.where(a >= b, a - b, a)


def div(a, b):
    return lax.div(a, jnp.int32(b))


def kernel(
    lat_hbm, mod_hbm, wqkv_hbm, wout_hbm, mask_ref, len_ref, out_ref,
    lat, mod, adapted, wqkv, kvsend, qsend, kv, q, acc, mx, sm, attsend, att, wcol, branch,
    in_sem, w_sem, kvs_sem, qs_sem, kv_sem, q_sem, b_sem, c_sem, att_sem, x_sem, wos_sem, wor_sem,
):
    t_id = lax.axis_index("tm")
    z, y = div(t_id, NY), rem(t_id, NY)
    m = lax.axis_index("mp")
    c = lax.axis_index("dec")
    yp, ym, y2 = wrap(y + 1, NY), wrap(y + NY - 1, NY), wrap(y + 2, NY)
    xp, xm, x2 = wrap(m + 1, NX), wrap(m + NX - 1, NX), wrap(m + 2, NX)
    width = wout_hbm.shape[0]
    row_core = div(z, 4)
    row_u = 3 * row_core + rem(z, 4)
    active = rem(z, 4) != 3
    q_core = rem(div(z + 1, 2), 2)
    slab_core = rem(z, 2)

    rel = wrap(z - 4 * c + NZ, NZ)
    first = jnp.where(rel == 1, 1, jnp.where((rel >= 2) & (rel <= 4), 2, 0))
    second = jnp.where(rel == 1, 0, jnp.where(rel == 5, 2, 1))

    def nearest(i):
        return jnp.where(i == 0, first, jnp.where(i == 1, second, 3 - first - second))

    def at(z_=z, y_=y, m_=m, c_=c):
        return {"tm": z_ * NY + y_, "mp": m_, "dec": c_}

    def remote(src, dst, ssem, rsem, device):
        return pltpu.make_async_remote_copy(
            src_ref=src, dst_ref=dst, send_sem=ssem, recv_sem=rsem,
            device_id=device, device_id_type=pl.DeviceIdType.MESH,
        )

    lat_copy = pltpu.make_async_copy(lat_hbm, lat, in_sem.at[0])
    mod_copy = pltpu.make_async_copy(mod_hbm, mod, in_sem.at[1])
    lat_copy.start()
    mod_copy.start()

    barrier = pltpu.get_barrier_semaphore()
    partners = [at(c_=1 - c), at(y_=yp), at(y_=ym)]
    for dz in range(1, NZ):
        for cc in range(2):
            partners.append(at(z_=wrap(z + dz, NZ), c_=jnp.int32(cc)))
    for dx in range(1, NX):
        for cc in range(2):
            partners.append(at(m_=wrap(m + dx, NX), c_=jnp.int32(cc)))
    for device in partners:
        pl.semaphore_signal(barrier, inc=1, device_id=device, device_id_type=pl.DeviceIdType.MESH)

    def weight_copy(k, part):
        cols = pl.ds(pl.multiple_of(k * HS, HS), HS)
        return pltpu.make_async_copy(
            wqkv_hbm.at[(part + 1) % 3, :, cols], wqkv.at[k, :, pl.ds(part * HS, HS)], w_sem.at[k]
        )

    for i in range(3):
        for part in range(3):
            weight_copy(nearest(i), part).start()
    own_cols = pl.ds(pl.multiple_of((2 * m + c) * width, HS), width)
    own_rows = pl.ds(pl.multiple_of(c * width, HS), width)
    wout_copy = pltpu.make_async_copy(wout_hbm.at[:, own_cols], wcol.at[m, own_rows, :], in_sem.at[2])
    wout_copy.start()

    mx[...] = jnp.full(mx.shape, NEG, jnp.float32)
    sm[...] = jnp.zeros(sm.shape, jnp.float32)
    acc[...] = jnp.zeros(acc.shape, jnp.float32)

    with jax.named_scope("load"):
        lat_copy.wait()
        mod_copy.wait()
    rows = 16

    @pl.loop(0, TOK // rows, unroll=4)
    def _(r):
        block = pl.ds(pl.multiple_of(r * rows, rows), rows)
        wide = lat[block, :].astype(jnp.float32)
        centred = wide - jnp.mean(wide, axis=-1, keepdims=True)
        var = jnp.mean(centred * centred, axis=-1, keepdims=True)
        normed = centred * lax.rsqrt(var + 1e-06)
        adapted[block, :] = (normed * (1.0 + mod[1]) + mod[0]).astype(jnp.bfloat16)

    with jax.named_scope("entry"):
        pl.semaphore_wait(barrier, len(partners))

    def wout_send(dx, dc):
        m_, c_ = wrap(m + dx, NX), (1 - c if dc else c)
        cols = pl.ds(pl.multiple_of((2 * m_ + c_) * width, HS), width)
        return remote(
            wout_hbm.at[:, cols], wcol.at[m, own_rows, :],
            wos_sem.at[0], wor_sem.at[0], at(m_=m_, c_=c_),
        )

    others = [(dx, dc) for dx in range(NX) for dc in range(2) if (dx, dc) != (0, 0)]

    def piece(s, p, start=0, size=TOK):
        return kv.at[s, pl.ds(pl.multiple_of(p * TOK + start, HALF), size), :]

    def kv_remote(k):
        return remote(kvsend.at[k], piece(z, y), kvs_sem.at[k], kv_sem.at[z, y, 0], at(z_=4 * c + k, c_=slab_core))

    def q_remote(k):
        return remote(qsend.at[k], q.at[div(z, 2)], qs_sem.at[k], q_sem.at[div(z, 2)], at(z_=4 * c + k, c_=q_core))

    def hop(s, slot):
        p, device, half = (
            (y, at(y_=yp), None), (y, at(y_=ym), None), (y, at(c_=1 - c), None),
            (ym, at(y_=yp), 0), (ym, at(c_=1 - c), None),
            (yp, at(y_=ym), 1), (yp, at(c_=1 - c), None),
            (y2, at(c_=1 - c), None),
        )[slot]
        start, size = (0, TOK) if half is None else (half * HALF, HALF)
        ref = piece(s, p, start, size)
        return remote(ref, ref, b_sem.at[0], kv_sem.at[s, p, half or 0], device)

    def kv_local(k):
        return (4 * c + k == z) & (slab_core == c)

    def q_local(k):
        return (4 * c + k == z) & (q_core == c)

    def send_phase(phase, i):
        k = nearest(i)
        away = wrap(4 * c + k - z + NZ, NZ)
        far = jnp.maximum(jnp.minimum(away, NZ - away), 1)

        @pl.when((far == phase) & jnp.logical_not(kv_local(k)))
        def _():
            kv_remote(k).start()

        @pl.when((jnp.maximum(far - 1, 1) == phase) & jnp.logical_not(q_local(k)))
        def _():
            q_remote(k).start()

    def send_rest(phase):
        @pl.loop(0, 3)
        def _(i):
            send_phase(phase, i)

    @pl.loop(0, 3)
    def _(i):
        k = nearest(i)
        with jax.named_scope("weights"):
            pltpu.make_async_copy(wqkv.at[k], wqkv.at[k], w_sem.at[k]).wait()
        made = jnp.dot(adapted[...], wqkv[k], preferred_element_type=jnp.float32)
        kvsend[k] = made[:, 0:2 * HS].astype(jnp.bfloat16)
        qsend[k] = (made[:, 2 * HS:3 * HS] * (1.0 / HS**0.5)).astype(jnp.bfloat16)

        @pl.when(kv_local(k))
        def _():
            kv[z, pl.ds(pl.multiple_of(y * TOK, TOK), TOK), :] = kvsend[k]

        @pl.when(q_local(k))
        def _():
            q[div(z, 2)] = qsend[k]

        @pl.when((i == 0) & kv_local(k))
        def _():
            for slot in range(3):
                hop(z, slot).start()

        send_phase(1, i)

        @pl.when(i == 0)
        def _():
            for pair in others:
                wout_send(*pair).start()

    def order(t):
        return wrap(z + jnp.where(rem(t, 2) == 1, NZ - div(t + 1, 2), div(t + 1, 2)), NZ)

    def group_row(k):
        return 2 * k + (1 - c if k % 2 else c)

    def q_here(k):
        return (group_row(k) == z) & (row_core == c)

    def kv_wait(s, p, half=0, size=TOK):
        start = half * HALF if size == HALF else 0
        ref = piece(s, p, start, size)
        remote(ref, ref, b_sem.at[0], kv_sem.at[s, p, half], at(c_=1 - c)).wait_recv()

    def relay(t, k, rows, mine):
        if k == 0:
            @pl.when((t < NZ) & mine[0])
            def _():
                s = rows[0]

                @pl.when(jnp.logical_not((t == 0) & (row_core == c)))
                def _():
                    with jax.named_scope("wait_z"):
                        kv_wait(s, y)

                @pl.when(jnp.logical_not((t == 0) & (row_core == c)))
                def _():
                    for slot in range(3):
                        hop(s, slot).start()

            @pl.when((t >= 3) & jnp.logical_not(mine[3]))
            def _():
                with jax.named_scope("wait_core"):
                    for p in range(NY):
                        kv_wait(rows[3], jnp.int32(p))

        if k == 1:
            @pl.when((t >= 1) & (t < NZ + 1) & mine[1])
            def _():
                with jax.named_scope("wait_ym"):
                    kv_wait(rows[1], ym)
                hop(rows[1], 3).start()
                hop(rows[1], 4).start()

        if k == 2:
            @pl.when((t >= 1) & (t < NZ + 1) & mine[1])
            def _():
                with jax.named_scope("wait_yp"):
                    kv_wait(rows[1], yp)
                hop(rows[1], 5).start()
                hop(rows[1], 6).start()

        if k == 3:
            @pl.when((t >= 2) & (t < NZ + 2) & mine[2])
            def _():
                with jax.named_scope("wait_y2"):
                    kv_wait(rows[2], y2, 0, HALF)
                    kv_wait(rows[2], y2, 1, HALF)
                hop(rows[2], 7).start()

    def tile(k, s):
        group = group_row(k) * NY + y
        lane = lax.broadcasted_iota(jnp.int32, (1, TOK), 1)
        parts = []
        for p in range(NY):
            key_group = s * NY + p
            limit = jnp.where(mask_ref[group, key_group] == 1, len_ref[key_group], 0)
            parts.append(jnp.where(lane < limit, 0.0, NEG).astype(jnp.float32))
        bias = jnp.concatenate(parts, axis=1)
        score = lax.dot_general(
            q[k], kv[s, :, 0:HS], (((1,), (1,)), ((), ())), preferred_element_type=jnp.float32
        ) + bias
        old = mx[k]
        new = jnp.maximum(old, jnp.max(score, axis=-1, keepdims=True))
        keep = jnp.exp(old - new)
        weight = jnp.exp(score - new[:, 0:1])
        mx[k] = new
        total = weight[:, 0:HS]
        for i in range(1, NY * TOK // HS):
            total += weight[:, i * HS:(i + 1) * HS]
        sm[k] = sm[k] * keep + total
        acc[k] = acc[k] * keep + jnp.dot(
            weight.astype(jnp.bfloat16), kv[s, :, HS:2 * HS], preferred_element_type=jnp.float32
        )

    def att_piece(x, u, half=None):
        start, size = (0, TOK) if half is None else (half * HALF, HALF)
        return att.at[x, pl.ds(start, size), pl.ds(pl.multiple_of(u * HS, HS), HS)]

    def att_remote(k):
        return remote(
            attsend.at[k], att_piece(m, row_u), c_sem.at[k], att_sem.at[m, row_u, 0],
            at(z_=group_row(k), c_=row_core),
        )

    def slot_steps(k, by_distance):
        row = group_row(k)
        away = wrap(row - z + NZ, NZ)
        rank = jnp.where(away <= 3, 2 * away, jnp.where(away == 4, NZ - 1, 2 * (NZ - away) - 1))
        begin = jnp.maximum(rank - 2, 0)
        last = begin
        for i, s in enumerate(by_distance):
            last = jnp.where((s <= row) & (i > last), i, last)
        return row, begin, last

    def compute(j, k, s_now, steps):
        row, begin, last = steps

        @pl.when((j == begin) & jnp.logical_not(q_here(k)))
        def _():
            with jax.named_scope("wait_q"):
                remote(q.at[k], q.at[k], c_sem.at[k], q_sem.at[k], at(c_=1 - c)).wait_recv()

        @pl.when(j >= begin)
        def _():
            @pl.loop(jnp.where(j == begin, 0, j), j + 1)
            def _(i):
                s = jnp.where(i == j, s_now, order(i))

                @pl.when(s <= row)
                def _():
                    with jax.named_scope("tile"):
                        tile(k, s)

        @pl.when(j == last)
        def _():
            done = (acc[k] / jnp.sum(sm[k], axis=-1, keepdims=True)).astype(jnp.bfloat16)

            @pl.when(q_here(k))
            def _():
                att[m, :, pl.ds(pl.multiple_of(row_u * HS, HS), HS)] = done

            @pl.when(jnp.logical_not(q_here(k)))
            def _():
                attsend[k] = done
                att_remote(k).start()

    @pl.when(active)
    def _():
        by_distance = [wrap(z + (NZ - (i + 1) // 2 if i % 2 else i // 2), NZ) for i in range(NZ)]
        steps = [slot_steps(k, by_distance) for k in range(4)]

        def step(t, earlier):
            rows = (order(t),) + earlier
            mine = [rem(s, 2) == c for s in rows]
            for k in range(4):
                relay(t, k, rows, mine)
                if k == 0:
                    @pl.when(t == 0)
                    def _():
                        pl.delay(PAUSE)
                        send_rest(2)

                    @pl.when(t == 3)
                    def _():
                        send_rest(3)

                if k == 1:
                    @pl.when(t == 4)
                    def _():
                        send_rest(4)

                @pl.when(t >= 3)
                def _():
                    compute(t - 3, k, rows[3], steps[k])

            return rows[:3]

        lax.fori_loop(0, NZ + 3, step, (z, z, z))

    @pl.when(jnp.logical_not(active))
    def _():
        pl.delay(PAUSE)
        send_rest(2)
        pl.delay(5 * PAUSE // 2)
        send_rest(3)

    def att_wait(x, u, half=None):
        ref = att_piece(x, u, half)
        remote(ref, ref, x_sem.at[0], att_sem.at[x, u, half or 0], at(c_=1 - c)).wait_recv()

    def att_hop(k, slot):
        u = 3 * c + k
        x, device, half = (
            (m, at(m_=xp), None), (m, at(m_=xm), None), (m, at(c_=1 - c), None),
            (xm, at(m_=xp), 0), (xm, at(c_=1 - c), None),
            (xp, at(m_=xm), 1), (xp, at(c_=1 - c), None),
            (x2, at(c_=1 - c), None), (m, at(m_=x2), None),
        )[slot]
        ref = att_piece(x, u, half)
        return remote(ref, ref, x_sem.at[0], att_sem.at[x, u, half or 0], device)

    def project(x, core):
        cols = pl.ds(pl.multiple_of(core * width, HS), width)
        with jax.named_scope("project"):
            return jnp.dot(att[x, :, cols], wcol[x, cols, :], preferred_element_type=jnp.float32)

    @pl.loop(0, 3)
    def _(k):
        @pl.when(jnp.logical_not(q_local(k)))
        def _():
            with jax.named_scope("wait_att"):
                att_wait(m, 3 * c + k)

        @pl.when(k == 2)
        def _():
            att_hop(k, 8).start()

        for slot in range(3):
            att_hop(k, slot).start()

    with jax.named_scope("wait_wout"):
        wout_copy.wait()
        seven = wqkv.at[0, pl.ds(0, 7 * width), pl.ds(0, width)]
        remote(seven, seven, wos_sem.at[0], wor_sem.at[0], at(c_=1 - c)).wait_recv()
    branch[...] = project(m, c)

    @pl.loop(0, 3)
    def _(k):
        with jax.named_scope("wait_xm"):
            att_wait(xm, 3 * c + k)
        @pl.when(k < 2)
        def _():
            att_hop(k, 3).start()

        att_hop(k, 4).start()
        with jax.named_scope("wait_xp"):
            att_wait(xp, 3 * c + k)
        @pl.when(k < 2)
        def _():
            att_hop(k, 5).start()

        att_hop(k, 6).start()

    def project_across(x):
        with jax.named_scope("wait_across"):
            for k in range(3):
                att_wait(x, 3 * (1 - c) + k)
        branch[...] += project(x, 1 - c)

    project_across(m)
    branch[...] += project(xm, c)
    branch[...] += project(xp, c)

    @pl.loop(0, 3)
    def _(k):
        with jax.named_scope("wait_x2"):
            @pl.when(k < 2)
            def _():
                att_wait(x2, 3 * c + k, 0)
                att_wait(x2, 3 * c + k, 1)

            @pl.when(k == 2)
            def _():
                att_wait(x2, 3 * c + k)

        att_hop(k, 7).start()

    project_across(xm)
    project_across(xp)
    branch[...] += project(x2, c)
    project_across(x2)

    with jax.named_scope("final"):
        wide = lat[:, own_cols].astype(jnp.float32)
        out_ref[...] = (wide + mod[2, :, own_cols] * branch[...]).astype(jnp.bfloat16)

    def all_left(ref, sem):
        remote(ref, ref, sem, wor_sem.at[0], at(c_=1 - c)).wait_send()

    with jax.named_scope("leave"):
        all_left(wqkv.at[0, pl.ds(0, 7 * width), pl.ds(0, width)], wos_sem.at[0])
        all_left(adapted.at[:, pl.ds(0, 21 * HS)], x_sem.at[0])

    @pl.loop(0, 3)
    def _(k):
        @pl.when(jnp.logical_not(kv_local(k)))
        def _():
            kv_remote(k).wait_send()

        @pl.when(jnp.logical_not(q_local(k)))
        def _():
            q_remote(k).wait_send()

    @pl.when(active)
    def _():
        all_left(kv.at[pl.ds(0, 7)], b_sem.at[0])

        for k in range(4):
            @pl.when(jnp.logical_not(q_here(k)))
            def _():
                att_remote(k).wait_send()


def shards(latents, modulation, w_qkv, w_out, block_mask, lengths):
    tok, d = latents.shape
    width = w_out.shape[0]
    dma = pltpu.SemaphoreType.DMA
    vmem = pltpu.VMEM
    bf16, f32 = jnp.bfloat16, jnp.float32
    anywhere = pl.BlockSpec(memory_space=pl.ANY)
    scalars = pl.BlockSpec(memory_space=pltpu.SMEM)
    return pl.pallas_call(
        kernel,
        out_shape=pltpu.VMEM((tok, width), bf16),
        in_specs=[anywhere] * 4 + [scalars] * 2,
        out_specs=pl.BlockSpec(memory_space=pltpu.VMEM),
        scratch_shapes=[
            vmem((tok, d), bf16), vmem((3, 1, d), f32), vmem((tok, d), bf16),
            vmem((3, d, 3 * HS), bf16), vmem((3, tok, 2 * HS), bf16), vmem((3, tok, HS), bf16),
            vmem((NZ, NY * tok, 2 * HS), bf16), vmem((4, tok, HS), bf16),
            vmem((4, tok, HS), f32), vmem((4, tok, HS), f32), vmem((4, tok, HS), f32),
            vmem((4, tok, HS), bf16), vmem((NX, tok, 6 * HS), bf16), vmem((NX, 2 * width, width), bf16),
            vmem((tok, width), f32),
            dma((3,)), dma((3,)), dma((3,)), dma((3,)), dma((NZ, NY, 2)), dma((4,)),
            dma((1,)), dma((4,)), dma((NX, 6, 2)), dma((1,)), dma((1,)), dma((1,)),
        ],
        compiler_params=pltpu.CompilerParams(
            collective_id=0, has_side_effects=True, vmem_limit_bytes=60 * 1024 * 1024
        ),
        name="attention_sublayer",
    )(latents, jnp.transpose(modulation, (1, 0, 2)), w_qkv, w_out, block_mask, lengths)


def solution(mesh):
    return jax.shard_map(
        shards,
        mesh=mesh,
        in_specs=(
            P("tm", None),
            P("tm", None, None),
            P(None, None, ("mp", "dec")),
            P(("mp", "dec"), None),
            P(),
            P(),
        ),
        out_specs=P("tm", ("mp", "dec")),
        check_vma=False,
    )
```
